16 devices in a mesh: pp: 2 (over z), ep: 8 (over y, x, core).
Axes of the slice: x: 2, y: 2, z: 2, core: 2. Of those that a mesh axis runs over, the one named last changes fastest.
Arguments:
- x_fwd: bfloat16 [2, 6144, 256], P('pp', 'ep')
- x_bwd: bfloat16 [2, 6144, 256], P('pp', 'ep')
- grad_in: bfloat16 [2, 6144, 256], P('pp', 'ep')
- dense_in: bfloat16 [2, 2, 256, 1024], P('pp')
- dense_out: bfloat16 [2, 2, 1024, 256], P('pp')
- exp_gate: bfloat16 [2, 2, 384, 256, 128], P('pp', None, 'ep')
- exp_up: bfloat16 [2, 2, 384, 256, 128], P('pp', None, 'ep')
- exp_down: bfloat16 [2, 2, 384, 128, 256], P('pp', None, 'ep')
- route_fwd: int32 [2, 2, 6144, 8], P('pp', None, 'ep')
- gate_fwd: bfloat16 [2, 2, 6144, 8], P('pp', None, 'ep')
- route_bwd: int32 [2, 2, 6144, 8], P('pp', None, 'ep')
- gate_bwd: bfloat16 [2, 2, 6144, 8], P('pp', None, 'ep')
Outputs:
- output 1: bfloat16 [2, 6144, 256], P('pp', 'ep')
- output 2: bfloat16 [2, 6144, 256], P('pp', 'ep')
- output 3: float32 [2, 2, 384, 256, 128], P('pp', None, 'ep')
- output 4: float32 [2, 2, 384, 256, 128], P('pp', None, 'ep')
- output 5: float32 [2, 2, 384, 128, 256], P('pp', None, 'ep')
All inputs are finite; a program needn't handle non-finite values.
Results may differ from the reference program's by a relative error of at most 0.02.
Values are sent between devices in bfloat16 or wider.
A program may use at most 1 GiB of HBM per device.

```python
import jax
import jax.numpy as jnp
from jax import lax

STAGES = 2
GROUPS = 8
TOKENS_DEV = 768
HIDDEN = 256
DENSE_FF = 1024
EXPERT_FF = 128
EXPERTS = 384
TOP_K = 8
CAPACITY = 2 * TOKENS_DEV * TOP_K // EXPERTS
NORM_EPS = 1e-6


def rms_norm(values):
    return values * lax.rsqrt(jnp.mean(values * values, axis=-1, keepdims=True) + NORM_EPS)


def rms_back(values, grad_out):
    inv_rms = lax.rsqrt(jnp.mean(values * values, axis=-1, keepdims=True) + NORM_EPS)
    proj_mean = jnp.mean(grad_out * values, axis=-1, keepdims=True)
    return inv_rms * grad_out - values * (inv_rms * inv_rms * inv_rms) * proj_mean


def silu_grad(pre_act):
    sig_value = jax.nn.sigmoid(pre_act)
    return sig_value * (1.0 + pre_act * (1.0 - sig_value))


def draw_route(key):
    key_order, key_shift, key_perm = jax.random.split(key, 3)
    half_cap = CAPACITY // 2
    expert_order = jax.random.permutation(key_order, EXPERTS)
    pair_shift = jax.random.randint(key_shift, (EXPERTS // 2,), 0, half_cap + 1).at[0].set(half_cap)
    counts = jnp.full((EXPERTS,), half_cap, jnp.int32).at[expert_order[0::2]].add(pair_shift).at[expert_order[1::2]].add(-pair_shift)
    run_ends = jnp.cumsum(counts)
    positions = jnp.arange(TOKENS_DEV * TOP_K, dtype=jnp.int32)
    expert_ids = jnp.searchsorted(run_ends, positions, side='right')
    slot_ids = positions - (run_ends - counts)[expert_ids]
    route_table = (expert_ids * CAPACITY + slot_ids).astype(jnp.int32).reshape(TOP_K, TOKENS_DEV).T
    return route_table[jax.random.permutation(key_perm, TOKENS_DEV)]


def draw_routes(key):
    keys = jax.random.split(key, STAGES * 2 * GROUPS)
    return jax.vmap(draw_route)(keys).reshape(STAGES, 2, GROUPS * TOKENS_DEV, TOP_K)


def setup_inputs(seed: int = 0) -> dict:
    keys = jax.random.split(jax.random.key(seed), 12)
    tok_shape = (STAGES, GROUPS * TOKENS_DEV, HIDDEN)
    route_shape = (STAGES, 2, GROUPS * TOKENS_DEV, TOP_K)
    up_shape = (STAGES, 2, EXPERTS, HIDDEN, EXPERT_FF)
    down_shape = (STAGES, 2, EXPERTS, EXPERT_FF, HIDDEN)

    def normal_bf16(key, shape, scale):
        return (jax.random.normal(key, shape, jnp.float32) * scale).astype(jnp.bfloat16)

    def gate_draw(key):
        return (jax.random.uniform(key, route_shape, jnp.float32, 0.05, 1.95) * (2.0 * TOP_K ** -0.5)).astype(jnp.bfloat16)

    return dict(
        x_fwd=normal_bf16(keys[0], tok_shape, 1.0),
        x_bwd=normal_bf16(keys[1], tok_shape, 1.0),
        grad_in=normal_bf16(keys[2], tok_shape, 1.0),
        dense_in=normal_bf16(keys[3], (STAGES, 2, HIDDEN, DENSE_FF), HIDDEN ** -0.5),
        dense_out=normal_bf16(keys[4], (STAGES, 2, DENSE_FF, HIDDEN), DENSE_FF ** -0.5),
        exp_gate=normal_bf16(keys[5], up_shape, HIDDEN ** -0.5),
        exp_up=normal_bf16(keys[6], up_shape, HIDDEN ** -0.5),
        exp_down=normal_bf16(keys[7], down_shape, EXPERT_FF ** -0.5),
        route_fwd=draw_routes(keys[8]),
        gate_fwd=gate_draw(keys[9]),
        route_bwd=draw_routes(keys[10]),
        gate_bwd=gate_draw(keys[11]),
    )


def to_slots(rows, route):
    def one_source(src_rows, src_route):
        table = jnp.zeros((EXPERTS * CAPACITY, HIDDEN), src_rows.dtype)
        return table.at[src_route.reshape(-1)].set(src_rows.reshape(-1, HIDDEN))
    return jax.vmap(one_source)(rows, route).reshape(GROUPS, EXPERTS, CAPACITY, HIDDEN)


def from_slots(table, route):
    flat = table.reshape(GROUPS, EXPERTS * CAPACITY, HIDDEN)
    return jax.vmap(lambda src_table, src_route: src_table[src_route])(flat, route)


def dense_forward(tokens, w_in, w_out):
    normed = rms_norm(tokens.astype(jnp.float32)).astype(jnp.bfloat16)
    pre_act = jnp.dot(normed, w_in, preferred_element_type=jnp.float32)
    mid_act = jax.nn.silu(pre_act).astype(jnp.bfloat16)
    hidden = (tokens.astype(jnp.float32) + jnp.dot(mid_act, w_out, preferred_element_type=jnp.float32)).astype(jnp.bfloat16)
    return pre_act, hidden


def block_front(tokens, route, weights):
    w_in, w_out, w_gate, w_up, w_down = weights
    flat = tokens.reshape(GROUPS * TOKENS_DEV, HIDDEN)
    pre_act, hidden = dense_forward(flat, w_in, w_out)
    normed = rms_norm(hidden.astype(jnp.float32)).astype(jnp.bfloat16)
    spread = jnp.broadcast_to(normed.reshape(GROUPS, TOKENS_DEV, 1, HIDDEN), (GROUPS, TOKENS_DEV, TOP_K, HIDDEN))
    slots = to_slots(spread, route).astype(jnp.float32)
    gate_pre = jnp.einsum('gecd,edf->gecf', slots, w_gate.astype(jnp.float32))
    up_pre = jnp.einsum('gecd,edf->gecf', slots, w_up.astype(jnp.float32))
    expert_mid = (jax.nn.silu(gate_pre) * up_pre).astype(jnp.bfloat16)
    return flat, pre_act, hidden, slots, gate_pre, up_pre, expert_mid


def block_finish(saved, route, gate, weights):
    hidden = saved[2]
    expert_mid = saved[6]
    expert_out = jnp.einsum('gecf,efd->gecd', expert_mid.astype(jnp.float32), weights[4].astype(jnp.float32)).astype(jnp.bfloat16)
    picked = from_slots(expert_out, route)
    mixed = jnp.einsum('gtk,gtkd->gtd', gate.astype(jnp.float32), picked.astype(jnp.float32))
    return (hidden.reshape(GROUPS, TOKENS_DEV, HIDDEN).astype(jnp.float32) + mixed).astype(jnp.bfloat16)


def block_backward(grad_out, saved, route, gate, weights):
    w_in, w_out, w_gate, w_up, w_down = weights
    flat, pre_act, hidden, slots, gate_pre, up_pre, expert_mid = saved
    grad_send = (gate.astype(jnp.float32)[..., None] * grad_out.astype(jnp.float32)[:, :, None, :]).astype(jnp.bfloat16)
    grad_slots = to_slots(grad_send, route).astype(jnp.float32)
    grad_mid = jnp.einsum('gecd,efd->gecf', grad_slots, w_down.astype(jnp.float32))
    grad_gate_pre = (grad_mid * up_pre * silu_grad(gate_pre)).astype(jnp.bfloat16).astype(jnp.float32)
    grad_up_pre = (grad_mid * jax.nn.silu(gate_pre)).astype(jnp.bfloat16).astype(jnp.float32)
    dw_down = jnp.einsum('gecf,gecd->efd', expert_mid.astype(jnp.float32), grad_slots)
    dw_gate = jnp.einsum('gecd,gecf->edf', slots, grad_gate_pre)
    dw_up = jnp.einsum('gecd,gecf->edf', slots, grad_up_pre)
    grad_rows = (jnp.einsum('gecf,edf->gecd', grad_gate_pre, w_gate.astype(jnp.float32)) + jnp.einsum('gecf,edf->gecd', grad_up_pre, w_up.astype(jnp.float32))).astype(jnp.bfloat16)
    grad_norm = jnp.sum(from_slots(grad_rows, route).astype(jnp.float32), axis=2).reshape(GROUPS * TOKENS_DEV, HIDDEN)
    grad_hidden = grad_out.reshape(GROUPS * TOKENS_DEV, HIDDEN).astype(jnp.float32) + rms_back(hidden.astype(jnp.float32), grad_norm)
    grad_dense = jnp.dot(grad_hidden.astype(jnp.bfloat16), w_out.T, preferred_element_type=jnp.float32)
    grad_pre = (grad_dense * silu_grad(pre_act)).astype(jnp.bfloat16)
    grad_act = jnp.dot(grad_pre, w_in.T, preferred_element_type=jnp.float32)
    grad_tokens = (grad_hidden + rms_back(flat.astype(jnp.float32), grad_act)).astype(jnp.bfloat16)
    return grad_tokens.reshape(GROUPS, TOKENS_DEV, HIDDEN), dw_gate, dw_up, dw_down


def stage_step(operands):
    x_fwd, x_bwd, grad_in, dense_in, dense_out, exp_gate, exp_up, exp_down, route_fwd, gate_fwd, route_bwd, gate_bwd = operands
    tok_shape = (GROUPS, TOKENS_DEV, HIDDEN)
    route_shape = (2, GROUPS, TOKENS_DEV, TOP_K)
    route_f = route_fwd.reshape(route_shape)
    gate_f = gate_fwd.reshape(route_shape)
    route_b = route_bwd.reshape(route_shape)
    gate_b = gate_bwd.reshape(route_shape)
    weights = [(dense_in[block], dense_out[block], exp_gate[block], exp_up[block], exp_down[block]) for block in range(2)]
    tokens = x_fwd.reshape(tok_shape)
    for block in range(2):
        saved = block_front(tokens, route_f[block], weights[block])
        tokens = block_finish(saved, route_f[block], gate_f[block], weights[block])
    saved_first = block_front(x_bwd.reshape(tok_shape), route_b[0], weights[0])
    mid_tokens = block_finish(saved_first, route_b[0], gate_b[0], weights[0])
    saved_second = block_front(mid_tokens, route_b[1], weights[1])
    grad_mid, wg_two, wu_two, wd_two = block_backward(grad_in.reshape(tok_shape), saved_second, route_b[1], gate_b[1], weights[1])
    grad_first, wg_one, wu_one, wd_one = block_backward(grad_mid, saved_first, route_b[0], gate_b[0], weights[0])
    return (tokens.reshape(GROUPS * TOKENS_DEV, HIDDEN), grad_first.reshape(GROUPS * TOKENS_DEV, HIDDEN), jnp.stack([wg_one, wg_two]), jnp.stack([wu_one, wu_two]), jnp.stack([wd_one, wd_two]))


def reference(x_fwd, x_bwd, grad_in, dense_in, dense_out, exp_gate, exp_up, exp_down, route_fwd, gate_fwd, route_bwd, gate_bwd):
    results = lax.map(stage_step, (x_fwd, x_bwd, grad_in, dense_in, dense_out, exp_gate, exp_up, exp_down, route_fwd, gate_fwd, route_bwd, gate_bwd))
    y_out, dx_out, dw_gate, dw_up, dw_down = results
    return jnp.roll(y_out, 1, axis=0), jnp.roll(dx_out, -1, axis=0), dw_gate, dw_up, dw_down
```

```python
import jax
import jax.numpy as jnp
from jax import lax
from jax.experimental import pallas as pl
from jax.experimental.pallas import tpu as pltpu
from jax.sharding import PartitionSpec as P

MESH = pl.DeviceIdType.MESH
EPS = 1e-6
F32, BF16, I32 = jnp.float32, jnp.bfloat16, jnp.int32
T, D, FF, K = 768, 256, 1024, 8
G, E, C, F = 8, 48, 32, 128
S = E * C
NJ = S // 128
HALF = T // 2
ROWS = 256
B1, FW1, B2, FW2 = 0, 1, 2, 3
QF, QB = 4, 2


def dot(a, b):
    return jnp.dot(a, b, preferred_element_type=F32)


def dot_nt(a, b):
    return lax.dot_general(a, b, (((1,), (1,)), ((), ())), preferred_element_type=F32)


def dot_tn(a, b):
    return lax.dot_general(a, b, (((0,), (0,)), ((), ())), preferred_element_type=F32)


def rms_norm(v):
    return v * lax.rsqrt(jnp.mean(v * v, axis=-1, keepdims=True) + EPS)


def rms_back(v, g):
    inv = lax.rsqrt(jnp.mean(v * v, axis=-1, keepdims=True) + EPS)
    proj = jnp.mean(g * v, axis=-1, keepdims=True)
    return inv * g - v * (inv * inv * inv) * proj


def xor1(a, b):
    return a + b - 2 * a * b


def kernel(xf_h, xb_h, gin_h, win_h, wout_h, eg_h, eu_h, ed_h, rt_v, gt_v,
           y_o, dx_o, gg_o, gu_o, gd_o, zs_o,
           zall, slots, trow, tb, w1, w2, xv, hv, yv,
           osib, sib_in, mine, tree_in, fin_in, wgu, wd, dgg, dgu, dgd,
           ag_s, ag_r, ag_f, tb_s, tb_r, sb_s, sb_r, tr_s, tr_r, fi_s, fi_r,
           w_sem, g_sem, l_sem, o_s, o_r):
    pp, me = lax.axis_index("pp"), lax.axis_index("ep")
    my_y, my_x, my_c = lax.div(me, 4), lax.rem(lax.div(me, 2), 2), lax.rem(me, 2)
    ZB, ZF, GB = 0, 1, 2
    SB, SF, RO = 0, 1, 2
    XB, XF, XB2 = 0, 1, 2
    HB1, HF, HB2 = 0, 1, 2

    def peer(r):
        if isinstance(r, int):
            ry, rx, rc = r // 4, r // 2 % 2, r % 2
        else:
            ry, rx, rc = lax.div(r, 4), lax.rem(lax.div(r, 2), 2), lax.rem(r, 2)
        return xor1(my_y, ry) * 4 + xor1(my_x, rx) * 2 + xor1(my_c, rc)

    def dev(r):
        return {"pp": pp, "ep": peer(r)}

    def rcopy(src, dst, s_sem, r_sem, to):
        return pltpu.make_async_remote_copy(src_ref=src, dst_ref=dst, send_sem=s_sem, recv_sem=r_sem, device_id=to, device_id_type=MESH)

    barrier = pltpu.get_barrier_semaphore()
    for r in range(1, G):
        pl.semaphore_signal(barrier, inc=1, device_id=dev(r), device_id_type=MESH)
    stage_peer = {"pp": 1 - pp, "ep": me}
    pl.semaphore_signal(barrier, inc=1, device_id=stage_peer, device_id_type=MESH)

    local = [pltpu.make_async_copy(xb_h, xv.at[XB], l_sem.at[0]),
             pltpu.make_async_copy(xf_h, xv.at[XF], l_sem.at[1]),
             pltpu.make_async_copy(gin_h, zall.at[GB, me], l_sem.at[2]),
             pltpu.make_async_copy(win_h, w1, l_sem.at[3]),
             pltpu.make_async_copy(wout_h, w2, l_sem.at[4])]
    for c in local:
        c.start()
    local[0].wait()
    local[3].wait()
    local[4].wait()

    def ag_send(i, buf):
        block = zall.at[buf, me]
        for r in (6, 2, 4, 1):
            rcopy(block, block, ag_s.at[i, r], ag_r.at[i, r], dev(r)).start()

    def ag_wait(i, buf, r):
        src = zall.at[buf, peer(r)]
        rcopy(src, src, ag_s.at[i, r], ag_r.at[i, r], dev(1)).wait_recv()

        @pl.when(lax.rem(r, 2) == 0)
        def _():
            rcopy(src, src, ag_f.at[i, r], ag_r.at[i, r + 1], dev(1)).start()

    def ag_finish(i, buf):
        block = zall.at[buf, me]
        for r in (6, 2, 4, 1):
            rcopy(block, block, ag_s.at[i, r], ag_r.at[i, r], dev(r)).wait_send()
        for r in (2, 4, 6):
            src = zall.at[buf, peer(r)]
            rcopy(src, src, ag_f.at[i, r], ag_r.at[i, r + 1], dev(1)).wait_send()

    def dense_fwd(blk, x_ref, h_ref, z_ref):
        def body(i, _):
            rows = pl.ds(pl.multiple_of(i * ROWS, ROWS), ROWS)
            x = x_ref[rows, :].astype(F32)
            pre = dot(rms_norm(x).astype(BF16), w1[blk])
            h = (x + dot(jax.nn.silu(pre).astype(BF16), w2[blk])).astype(BF16)
            h_ref[rows, :] = h
            z_ref[rows, :] = rms_norm(h.astype(F32)).astype(BF16)
            return 0
        lax.fori_loop(0, T // ROWS, body, 0)

    def silu_grad(a):
        sig = jax.nn.sigmoid(a)
        return sig * (1.0 + a * (1.0 - sig))

    def dense_bwd(blk, x_ref, h_ref, g_ref, total, out_ref):
        def body(i, _):
            rows = pl.ds(pl.multiple_of(i * ROWS, ROWS), ROWS)
            x = x_ref[rows, :].astype(F32)
            pre = dot(rms_norm(x).astype(BF16), w1[blk])
            dh = g_ref[rows, :].astype(F32) + rms_back(h_ref[rows, :].astype(F32), total(rows))
            dm = dot_nt(dh.astype(BF16), w2[blk])
            dp = (dm * silu_grad(pre)).astype(BF16)
            out_ref[rows, :] = (dh + rms_back(x, dot_nt(dp, w1[blk]))).astype(BF16)
            return 0
        lax.fori_loop(0, T // ROWS, body, 0)

    def build_tables(first, last):
        def body(rt, _):
            acc_i = jnp.zeros((128, 128), F32)
            acc_g = jnp.zeros((128, 128), F32)
            for tc in range(T // 256):
                rows = rt_v[rt, :, tc * 256:(tc + 1) * 256]
                gates = gt_v[rt, :, tc * 256:(tc + 1) * 256]
                cols, gcols = rows.T, gates.T
                quad = lax.shift_right_logical(rows, 7)
                place = quad + 4 * lax.shift_right_logical(quad * 43, 9)
                lane = lax.bitwise_and(cols, 127)
                tok = lax.broadcasted_iota(I32, (256, 128), 0) + (tc * 256 + 1)
                low = lax.bitwise_and(tok, 255)
                high = (tok - low).astype(F32)
                low = low.astype(F32)
                lanes = lax.broadcasted_iota(I32, (256, 128), 1)
                spots = lax.broadcasted_iota(I32, (128, 256), 0)
                for k in range(K):
                    a = jnp.where(spots == place[k:k + 1, :], 1.0, 0.0).astype(BF16)
                    hit = lanes == lane[:, k:k + 1]
                    b = jnp.concatenate([jnp.where(hit, low, 0.0), jnp.where(hit, high, 0.0)], axis=1).astype(BF16)
                    both = dot(a, b)
                    acc_i += both[:, :128] + both[:, 128:]
                    acc_g += dot(a, jnp.where(hit, gcols[:, k:k + 1], 0.0).astype(BF16))
            trow[rt, :, 0] = acc_i.reshape(G, 16, 128)
            trow[rt, :, 1] = acc_g.reshape(G, 16, 128)
            tb[rt, me] = trow[rt, me]
            for r in range(1, G):
                rcopy(trow.at[rt, peer(r)], tb.at[rt, me], tb_s.at[rt, r], tb_r.at[rt, r], dev(r)).start()
            return 0
        lax.fori_loop(first, last, body, 0)

    def tables_wait(rt):
        for r in range(1, G):
            rcopy(trow.at[rt, peer(r)], tb.at[rt, peer(r)], tb_s.at[rt, r], tb_r.at[rt, r], dev(r)).wait()

    def dispatch(ag, buf, rt, dst, gated):
        def body(r, _):
            if ag is not None:
                @pl.when(r > 0)
                def _():
                    ag_wait(ag, buf, r)
            src = peer(r)
            z = zall[buf, src]
            cols = tb[rt, src, 0].T
            gcols = tb[rt, src, 1].T if gated else None
            base = pl.multiple_of(src * C, C)
            want = lax.broadcasted_iota(I32, (128, T), 1).astype(F32) + 1.0
            for j in range(0, NJ, 4):
                parts = []
                for q in range(j, j + 4):
                    val = gcols[:, q:q + 1] if gated else 1.0
                    parts.append(jnp.where(want == cols[:, q:q + 1], val, 0.0).astype(BF16))
                got = dot(jnp.concatenate(parts, axis=0), z).astype(BF16)
                slots[dst, 4 * j:4 * j + 16, pl.ds(base, C), :] = got.reshape(16, C, D)
            return 0
        lax.fori_loop(0, G, body, 0)
        if ag is not None:
            ag_finish(ag, buf)

    def w_copies(blk, i, slot, q):
        es = pl.ds(i * q, q)
        return [pltpu.make_async_copy(eg_h.at[blk, es], wgu.at[slot, pl.ds(0, q), :, pl.ds(0, F)], w_sem.at[slot, 0]),
                pltpu.make_async_copy(eu_h.at[blk, es], wgu.at[slot, pl.ds(0, q), :, pl.ds(F, F)], w_sem.at[slot, 1]),
                pltpu.make_async_copy(ed_h.at[blk, es], wd.at[slot, pl.ds(0, q)], w_sem.at[slot, 2])]

    def w_first(blk, q):
        for c in w_copies(blk, 0, 0, q):
            c.start()

    def experts_fwd(blk, src, dst):
        steps = E // QF

        def body(i, _):
            slot = lax.rem(i, 2)

            @pl.when(i + 1 < steps)
            def _():
                for c in w_copies(blk, i + 1, 1 - slot, QF):
                    c.start()
            for c in w_copies(blk, i, slot, QF):
                c.wait()
            for n in range(QF):
                e = i * QF + n
                gu = dot(slots[src, e], wgu[slot, n])
                mid = (jax.nn.silu(gu[:, :F]) * gu[:, F:]).astype(BF16)
                slots[dst, e] = dot(mid, wd[slot, n]).astype(BF16)
            return 0
        lax.fori_loop(0, steps, body, 0)

    def g_copies(blk, i, slot):
        es = pl.ds(i * QB, QB)
        return [pltpu.make_async_copy(dgg.at[slot], gg_o.at[blk, es], g_sem.at[slot, 0]),
                pltpu.make_async_copy(dgu.at[slot], gu_o.at[blk, es], g_sem.at[slot, 1]),
                pltpu.make_async_copy(dgd.at[slot], gd_o.at[blk, es], g_sem.at[slot, 2])]

    def experts_bwd(blk, zsrc, ro):
        steps = E // QB

        def body(i, _):
            slot = lax.rem(i, 2)

            @pl.when(i + 1 < steps)
            def _():
                for c in w_copies(blk, i + 1, 1 - slot, QB):
                    c.start()
            for c in w_copies(blk, i, slot, QB):
                c.wait()

            @pl.when(i >= 2)
            def _():
                for c in g_copies(blk, i - 2, slot):
                    c.wait()
            for n in range(QB):
                e = i * QB + n
                z, rr = slots[zsrc, e], slots[ro, e]
                gu = dot(z, wgu[slot, n])
                a, b = gu[:, :F], gu[:, F:]
                sig = jax.nn.sigmoid(a)
                act = a * sig
                mid = (act * b).astype(BF16)
                dm = dot_nt(rr, wd[slot, n])
                da = (dm * b * (sig * (1.0 + a * (1.0 - sig)))).astype(BF16)
                db = (dm * act).astype(BF16)
                dab = jnp.concatenate([da, db], axis=1)
                dgd[slot, n] = dot_tn(mid, rr)
                dw = dot_tn(z, dab)
                dgg[slot, n] = dw[:, :F]
                dgu[slot, n] = dw[:, F:]
                slots[ro, e] = dot_nt(dab, wgu[slot, n]).astype(BF16)
            for c in g_copies(blk, i, slot):
                c.start()
            return 0
        lax.fori_loop(0, steps, body, 0)
        for i in (steps - 2, steps - 1):
            for c in g_copies(blk, i, i % 2):
                c.wait()

    def combine(rs, ch, rt, src, gated):
        def rows_of(s):
            vals = slots[src, :, pl.ds(pl.multiple_of(s * C, C), C), :].reshape(S, D)
            want = lax.broadcasted_iota(I32, (T, 128), 0).astype(F32) + 1.0
            parts = []
            for j in range(NJ):
                val = tb[rt, s, 1, j:j + 1, :] if gated else 1.0
                parts.append(jnp.where(want == tb[rt, s, 0, j:j + 1, :], val, 0.0).astype(BF16))
            return dot(jnp.concatenate(parts, axis=1), vals)

        def sib_copy(q, n):
            return rcopy(osib.at[ch, n], sib_in.at[ch, q], sb_s.at[rs, q], sb_r.at[rs, q], dev(1))

        def body(n, _):
            q = 3 - n

            @pl.when(n >= 2)
            def _():
                sib_copy(q + 2, lax.rem(n, 2)).wait_send()
            osib[ch, lax.rem(n, 2)] = rows_of(peer(2 * q + 1))
            sib_copy(q, lax.rem(n, 2)).start()
            own = rows_of(peer(2 * q))
            sib_copy(q, lax.rem(n, 2)).wait_recv()
            mine[ch, q] = own + sib_in[ch, q]

            @pl.when(n == 0)
            def _():
                for c in tree(rs, ch):
                    c.start()

            @pl.when(n == 1)
            def _():
                fin(rs, ch, 1, 1).start()

            @pl.when(n == 2)
            def _():
                fin(rs, ch, 0, 0).start()
            return 0
        lax.fori_loop(0, 4, body, 0)
        for n in (2, 3):
            sib_copy(3 - n, n % 2).wait_send()
        first, second = tree(rs, ch)
        first.wait()
        mine[ch, 2, 0:HALF] += tree_in[ch, 0]
        fin(rs, ch, 1, 0).start()
        second.wait()
        mine[ch, 1, HALF:T] += tree_in[ch, 1]
        fin(rs, ch, 0, 1).start()

    def tree(rs, ch):
        return [rcopy(mine.at[ch, 3, pl.ds(0, HALF)], tree_in.at[ch, 0], tr_s.at[rs, 0], tr_r.at[rs, 0], dev(2)),
                rcopy(mine.at[ch, 3, pl.ds(HALF, HALF)], tree_in.at[ch, 1], tr_s.at[rs, 1], tr_r.at[rs, 1], dev(4))]

    def fin(rs, ch, axis, half):
        rows = pl.ds(half * HALF, HALF)
        return rcopy(mine.at[ch, 1 + axis, rows], fin_in.at[ch, axis, rows], fi_s.at[rs, axis, half], fi_r.at[rs, axis, half], dev(2 + 2 * axis))

    def rs_wait(rs, ch):
        for axis in range(2):
            for half in range(2):
                fin(rs, ch, axis, half).wait()

    def total_of(ch):
        return lambda rows: mine[ch, 0, rows, :] + fin_in[ch, 0, rows, :] + fin_in[ch, 1, rows, :]

    def block_out(ch, h_ref, out_ref):
        total = total_of(ch)

        def body(i, _):
            rows = pl.ds(pl.multiple_of(i * ROWS, ROWS), ROWS)
            out_ref[rows, :] = (h_ref[rows, :].astype(F32) + total(rows)).astype(BF16)
            return 0
        lax.fori_loop(0, T // ROWS, body, 0)

    w_first(0, QF)
    dense_fwd(0, xv.at[XB], hv.at[HB1], zall.at[ZB, me])
    pl.semaphore_wait(barrier, G)
    ag_send(0, ZB)
    build_tables(0, 1)
    local[1].wait()
    dense_fwd(0, xv.at[XF], hv.at[HF], zall.at[ZF, me])
    ag_send(1, ZF)
    local[2].wait()
    ag_send(2, GB)
    build_tables(1, 4)

    tables_wait(B1)
    dispatch(0, ZB, B1, SB, False)
    save = pltpu.make_async_copy(slots.at[SB], zs_o, l_sem.at[0])
    save.start()
    experts_fwd(0, SB, RO)
    w_first(0, QF)
    combine(0, 0, B1, RO, True)

    tables_wait(FW1)
    dispatch(1, ZF, FW1, SF, False)
    experts_fwd(0, SF, SF)
    w_first(1, QB)
    combine(1, 1, FW1, SF, True)

    rs_wait(0, 0)
    block_out(0, hv.at[HB1], xv.at[XB2])
    dense_fwd(1, xv.at[XB2], hv.at[HB2], zall.at[ZB, me])
    ag_send(3, ZB)
    tables_wait(B2)
    dispatch(2, GB, B2, RO, True)
    rs_wait(1, 1)
    block_out(1, hv.at[HF], xv.at[XF])
    dense_fwd(1, xv.at[XF], hv.at[HF], zall.at[ZF, me])
    ag_send(4, ZF)

    save.wait()
    dispatch(3, ZB, B2, SB, False)
    experts_bwd(1, SB, RO)
    w_first(1, QF)
    load = pltpu.make_async_copy(zs_o, slots.at[SB], l_sem.at[1])
    load.start()
    combine(2, 0, B2, RO, False)

    tables_wait(FW2)
    dispatch(4, ZF, FW2, SF, False)
    experts_fwd(1, SF, SF)
    w_first(0, QB)
    combine(3, 1, FW2, SF, True)

    rs_wait(2, 0)
    dense_bwd(1, xv.at[XB2], hv.at[HB2], zall.at[GB, me], total_of(0), zall.at[ZB, me])
    ag_send(5, ZB)
    rs_wait(3, 1)
    block_out(1, hv.at[HF], yv.at[0])
    send_y = rcopy(yv.at[0], y_o, o_s.at[0], o_r.at[0], stage_peer)
    send_y.start()

    dispatch(5, ZB, B1, RO, True)
    load.wait()
    experts_bwd(0, SB, RO)
    combine(4, 0, B1, RO, False)
    rs_wait(4, 0)
    dense_bwd(0, xv.at[XB], hv.at[HB1], zall.at[ZB, me], total_of(0), yv.at[1])
    send_x = rcopy(yv.at[1], dx_o, o_s.at[1], o_r.at[1], stage_peer)
    send_x.start()
    send_y.wait()
    send_x.wait()


def solution(mesh):
    def local_step(x_fwd, x_bwd, grad_in, dense_in, dense_out, exp_gate, exp_up, exp_down, route_fwd, gate_fwd, route_bwd, gate_bwd):
        route = jnp.stack([route_bwd[0, 0], route_fwd[0, 0], route_bwd[0, 1], route_fwd[0, 1]]).transpose(0, 2, 1)
        gate = jnp.stack([gate_bwd[0, 0], gate_fwd[0, 0], gate_bwd[0, 1], gate_fwd[0, 1]]).astype(F32).transpose(0, 2, 1)
        vmem, hbm = pl.BlockSpec(memory_space=pltpu.VMEM), pl.BlockSpec(memory_space=pl.ANY)
        dma = pltpu.SemaphoreType.DMA
        tok = jax.ShapeDtypeStruct((T, D), BF16)
        up = jax.ShapeDtypeStruct((2, E, D, F), F32)
        down = jax.ShapeDtypeStruct((2, E, F, D), F32)
        outs = pl.pallas_call(
            kernel,
            out_shape=(tok, tok, up, up, down, jax.ShapeDtypeStruct((E, G * C, D), BF16)),
            in_specs=[hbm] * 8 + [vmem] * 2,
            out_specs=(vmem, vmem, hbm, hbm, hbm, hbm),
            scratch_shapes=[
                pltpu.VMEM((3, G, T, D), BF16),
                pltpu.VMEM((3, E, G * C, D), BF16),
                pltpu.VMEM((4, G, 2, 16, 128), F32),
                pltpu.VMEM((4, G, 2, 16, 128), F32),
                pltpu.VMEM((2, D, FF), BF16),
                pltpu.VMEM((2, FF, D), BF16),
                pltpu.VMEM((3, T, D), BF16),
                pltpu.VMEM((3, T, D), BF16),
                pltpu.VMEM((2, T, D), BF16),
                pltpu.VMEM((2, 2, T, D), F32),
                pltpu.VMEM((2, 4, T, D), F32),
                pltpu.VMEM((2, 4, T, D), F32),
                pltpu.VMEM((2, 2, HALF, D), F32),
                pltpu.VMEM((2, 2, T, D), F32),
                pltpu.VMEM((2, QF, D, 2 * F), BF16),
                pltpu.VMEM((2, QF, F, D), BF16),
                pltpu.VMEM((2, QB, D, F), F32),
                pltpu.VMEM((2, QB, D, F), F32),
                pltpu.VMEM((2, QB, F, D), F32),
                dma((6, 8)), dma((6, 8)), dma((6, 8)),
                dma((4, 8)), dma((4, 8)),
                dma((5, 4)), dma((5, 4)), dma((5, 2)), dma((5, 2)), dma((5, 2, 2)), dma((5, 2, 2)),
                dma((2, 3)), dma((2, 3)), dma((5,)), dma((2,)), dma((2,)),
            ],
            compiler_params=pltpu.CompilerParams(collective_id=0, has_side_effects=True, vmem_limit_bytes=67043328),
        )(x_fwd[0], x_bwd[0], grad_in[0], dense_in[0], dense_out[0], exp_gate[0], exp_up[0], exp_down[0], route, gate)
        y_next, dx_prev, dgate, dup, ddown = outs[:5]
        return y_next[None], dx_prev[None], dgate[None], dup[None], ddown[None]

    tok_spec = P('pp', 'ep', None)
    dense_spec = P('pp', None, None, None)
    exp_spec = P('pp', None, 'ep', None, None)
    route_spec = P('pp', None, 'ep', None)
    return jax.shard_map(local_step, mesh=mesh, in_specs=(tok_spec, tok_spec, tok_spec, dense_spec, dense_spec, exp_spec, exp_spec, exp_spec, route_spec, route_spec, route_spec, route_spec), out_specs=(tok_spec, tok_spec, exp_spec, exp_spec, exp_spec), check_vma=False)
```

```python
import jax
import jax.numpy as jnp
from jax import lax
from jax.experimental import pallas as pl
from jax.experimental.pallas import tpu as pltpu
from jax.sharding import PartitionSpec as P

MESH = pl.DeviceIdType.MESH
EPS = 1e-6
F32, BF16, I32 = jnp.float32, jnp.bfloat16, jnp.int32
T, D, FF, K = 768, 256, 1024, 8
G, E, C, F = 8, 48, 32, 128
S = E * C
NJ = S // 128
HALF = T // 2
ROWS = 256
B1, FW1, B2, FW2 = range(4)
SIB, XN, YN, DIAG = 1, 2, 4, 6
LOW, UP = 0, 1
BB, FB = 0, 1
Q, AHEAD = 8, 2
STEPS = E // Q


def dot(a, b):
    return jnp.dot(a, b, preferred_element_type=F32)


def dot_nt(a, b):
    return lax.dot_general(a, b, (((1,), (1,)), ((), ())), preferred_element_type=F32)


def dot_tn(a, b):
    return lax.dot_general(a, b, (((0,), (0,)), ((), ())), preferred_element_type=F32)


def rms_norm(v):
    return v * lax.rsqrt(jnp.mean(v * v, axis=-1, keepdims=True) + EPS)


def rms_back(v, g):
    inv = lax.rsqrt(jnp.mean(v * v, axis=-1, keepdims=True) + EPS)
    proj = jnp.mean(g * v, axis=-1, keepdims=True)
    return inv * g - v * (inv * inv * inv) * proj


def xor1(a, b):
    return a + b - 2 * a * b


def kernel(xf_h, xb_h, gin_h, win_h, wout_h, eg_h, eu_h, ed_h, rt_v, gt_v,
           y_o, dx_o, z_o, r_o, dab_o, mid_o,
           zall, slots, trow, tb, w1, w2, xv, hv, yv,
           part, sib_in, tree_in, fin_in, wgu, wd, dab_v, mid_v,
           ag_s, ag_r, tb_s, tb_r, sb_s, sb_r, tr_s, tr_r, fi_s, fi_r,
           w_sem, g_sem, l_sem, o_s, o_r):
    pp, me = lax.axis_index("pp"), lax.axis_index("ep")
    my_y, my_x, my_c = lax.div(me, 4), lax.rem(lax.div(me, 2), 2), lax.rem(me, 2)
    ZB, ZF, GB = range(3)
    SB, SF, RO = range(3)
    XB, XF, XB2 = range(3)
    HB1, HF, HB2 = range(3)

    def peer(r):
        if isinstance(r, int):
            ry, rx, rc = r // 4, r // 2 % 2, r % 2
        else:
            ry, rx, rc = lax.div(r, 4), lax.rem(lax.div(r, 2), 2), lax.rem(r, 2)
        return xor1(my_y, ry) * 4 + xor1(my_x, rx) * 2 + xor1(my_c, rc)

    def dev(r):
        return {"pp": pp, "ep": peer(r)}

    def rcopy(src, dst, s_sem, r_sem, to):
        return pltpu.make_async_remote_copy(src_ref=src, dst_ref=dst, send_sem=s_sem, recv_sem=r_sem, device_id=to, device_id_type=MESH)

    barrier = pltpu.get_barrier_semaphore()
    for r in range(1, G):
        pl.semaphore_signal(barrier, inc=1, device_id=dev(r), device_id_type=MESH)
    stage_peer = {"pp": 1 - pp, "ep": me}
    pl.semaphore_signal(barrier, inc=1, device_id=stage_peer, device_id_type=MESH)

    pairs = [(xb_h, xv.at[XB]), (win_h, w1), (wout_h, w2), (xf_h, xv.at[XF]), (gin_h, zall.at[GB, me])]
    local = [pltpu.make_async_copy(src, dst, l_sem.at[n]) for n, (src, dst) in enumerate(pairs)]
    for c in local:
        c.start()
    load_xb, load_w1, load_w2, load_xf, load_g = local
    for c in (load_xb, load_w1, load_w2):
        c.wait()

    def half(buf, r, h):
        return zall.at[buf, me if r is None else peer(r), pl.ds(h * HALF, HALF)]

    def ag_copy(i, n, ref, r):
        return rcopy(ref, ref, ag_s.at[i, n], ag_r.at[i, n], dev(r))

    X_LOW, X_UP, Y_LOW, Y_UP, OWN, D_LOW, D_UP, PASS = range(8)

    def ag_own(i, buf):
        low, up = half(buf, None, LOW), half(buf, None, UP)
        return [ag_copy(i, X_LOW, low, XN), ag_copy(i, Y_UP, up, YN), ag_copy(i, X_UP, up, XN), ag_copy(i, Y_LOW, low, YN),
                ag_copy(i, OWN, zall.at[buf, me], SIB)]

    def ag_pass(i, buf):
        return ag_copy(i, D_LOW, half(buf, XN, LOW), YN), ag_copy(i, D_UP, half(buf, YN, UP), XN)

    def ag_sib(i, buf, n):
        return ag_copy(i, PASS + n, zall.at[buf, peer((XN, YN, DIAG)[n])], SIB)

    def ag_send(i, buf):
        for c in ag_own(i, buf):
            c.start()

    def ag_mid(i, buf):
        first, second = ag_pass(i, buf)
        ag_copy(i, X_LOW, half(buf, XN, LOW), XN).wait_recv()
        first.start()
        ag_copy(i, Y_UP, half(buf, YN, UP), YN).wait_recv()
        second.start()

    def ag_step(i, buf, r):
        waits = [[(OWN, zall.at[buf, peer(SIB)]), (X_UP, half(buf, XN, UP))],
                 [(PASS, zall.at[buf, peer(XN + SIB)]), (Y_LOW, half(buf, YN, LOW))],
                 [(PASS + 1, zall.at[buf, peer(YN + SIB)]), (D_LOW, half(buf, DIAG, LOW)), (D_UP, half(buf, DIAG, UP))],
                 [(PASS + 2, zall.at[buf, peer(DIAG + SIB)])]]
        for n, group in enumerate(waits):
            @pl.when(r == 2 * n + 1)
            def _(n=n, group=group):
                for sem, ref in group:
                    ag_copy(i, sem, ref, SIB).wait_recv()
                if len(group) > 1:
                    ag_sib(i, buf, n).start()

    def ag_finish(i, buf):
        for c in ag_own(i, buf) + list(ag_pass(i, buf)):
            c.wait_send()
        for n in range(3):
            ag_sib(i, buf, n).wait_send()

    def dense_fwd(blk, x_ref, h_ref, z_ref):
        def body(i, _):
            rows = pl.ds(pl.multiple_of(i * ROWS, ROWS), ROWS)
            x = x_ref[rows, :].astype(F32)
            pre = dot(rms_norm(x).astype(BF16), w1[blk])
            h = (x + dot(jax.nn.silu(pre).astype(BF16), w2[blk])).astype(BF16)
            h_ref[rows, :] = h
            z_ref[rows, :] = rms_norm(h.astype(F32)).astype(BF16)
            return 0
        lax.fori_loop(0, T // ROWS, body, 0)

    def silu_grad(a):
        sig = jax.nn.sigmoid(a)
        return sig * (1.0 + a * (1.0 - sig))

    def dense_bwd(blk, x_ref, h_ref, g_ref, total, out_ref):
        def body(i, _):
            rows = pl.ds(pl.multiple_of(i * ROWS, ROWS), ROWS)
            x = x_ref[rows, :].astype(F32)
            pre = dot(rms_norm(x).astype(BF16), w1[blk])
            dh = g_ref[rows, :].astype(F32) + rms_back(h_ref[rows, :].astype(F32), total(rows))
            dm = dot_nt(dh.astype(BF16), w2[blk])
            dp = (dm * silu_grad(pre)).astype(BF16)
            out_ref[rows, :] = (dh + rms_back(x, dot_nt(dp, w1[blk]))).astype(BF16)
            return 0
        lax.fori_loop(0, T // ROWS, body, 0)

    def build_tables(first, last):
        def body(rt, _):
            acc_i = jnp.zeros((128, 128), F32)
            acc_g = jnp.zeros((128, 128), F32)
            for tc in range(T // 256):
                rows = rt_v[rt, :, tc * 256:(tc + 1) * 256]
                gates = gt_v[rt, :, tc * 256:(tc + 1) * 256]
                cols, gcols = rows.T, gates.T
                quad = lax.shift_right_logical(rows, 7)
                place = quad + 4 * lax.shift_right_logical(quad * 43, 9)
                lane = lax.bitwise_and(cols, 127)
                tok = lax.broadcasted_iota(I32, (256, 128), 0) + (tc * 256 + 1)
                low = lax.bitwise_and(tok, 255)
                high = (tok - low).astype(F32)
                low = low.astype(F32)
                lanes = lax.broadcasted_iota(I32, (256, 128), 1)
                spots = lax.broadcasted_iota(I32, (128, 256), 0)
                for k in range(K):
                    a = jnp.where(spots == place[k:k + 1, :], 1.0, 0.0).astype(BF16)
                    hit = lanes == lane[:, k:k + 1]
                    b = jnp.concatenate([jnp.where(hit, low, 0.0), jnp.where(hit, high, 0.0)], axis=1).astype(BF16)
                    both = dot(a, b)
                    acc_i += both[:, :128] + both[:, 128:]
                    acc_g += dot(a, jnp.where(hit, gcols[:, k:k + 1], 0.0).astype(BF16))
            trow[rt, :, 0] = acc_i.reshape(G, 16, 128)
            trow[rt, :, 1] = acc_g.reshape(G, 16, 128)
            tb[rt, me] = trow[rt, me]
            return 0
        lax.fori_loop(first, last, body, 0)

    def tables_send(rt):
        for r in range(1, G):
            rcopy(trow.at[rt, peer(r)], tb.at[rt, me], tb_s.at[rt, r], tb_r.at[rt, r], dev(r)).start()

    def tables_wait(rt):
        for r in range(1, G):
            rcopy(trow.at[rt, peer(r)], tb.at[rt, peer(r)], tb_s.at[rt, r], tb_r.at[rt, r], dev(r)).wait()

    def dispatch(ag, buf, rt, dst, gated):
        def body(r, _):
            if ag is not None:
                ag_step(ag, buf, r)
            src = peer(r)
            z = zall[buf, src]
            cols = tb[rt, src, 0].T
            gcols = tb[rt, src, 1].T if gated else None
            base = pl.multiple_of(src * C, C)
            want = lax.broadcasted_iota(I32, (128, T), 1).astype(F32) + 1.0
            for j in range(0, NJ, 4):
                parts = []
                for q in range(j, j + 4):
                    val = gcols[:, q:q + 1] if gated else 1.0
                    parts.append(jnp.where(want == cols[:, q:q + 1], val, 0.0).astype(BF16))
                got = dot(jnp.concatenate(parts, axis=0), z).astype(BF16)
                slots[dst, 4 * j:4 * j + 16, pl.ds(base, C), :] = got.reshape(16, C, D)
            return 0
        lax.fori_loop(0, G, body, 0)
        if ag is not None:
            ag_finish(ag, buf)

    def w_copies(blk, i):
        slot = i % (AHEAD + 1) if isinstance(i, int) else lax.rem(i, AHEAD + 1)
        es = pl.ds(i * Q, Q)
        return [pltpu.make_async_copy(eg_h.at[blk, es], wgu.at[slot, :, :, pl.ds(0, F)], w_sem.at[slot, 0]),
                pltpu.make_async_copy(eu_h.at[blk, es], wgu.at[slot, :, :, pl.ds(F, F)], w_sem.at[slot, 1]),
                pltpu.make_async_copy(ed_h.at[blk, es], wd.at[slot], w_sem.at[slot, 2])]

    def w_first(blk):
        for i in range(AHEAD):
            for c in w_copies(blk, i):
                c.start()

    def w_next(blk, i):
        @pl.when(i + AHEAD < STEPS)
        def _():
            for c in w_copies(blk, i + AHEAD):
                c.start()
        for c in w_copies(blk, i):
            c.wait()
        return lax.rem(i, AHEAD + 1)

    def experts_fwd(blk, src, dst):
        def body(i, _):
            slot = w_next(blk, i)
            es = [i * Q + n for n in range(Q)]
            gus = [dot(slots[src, e], wgu[slot, n]) for n, e in enumerate(es)]
            mids = [(jax.nn.silu(gu[:, :F]) * gu[:, F:]).astype(BF16) for gu in gus]
            outs = [dot(mid, wd[slot, n]).astype(BF16) for n, mid in enumerate(mids)]
            for e, out in zip(es, outs):
                slots[dst, e] = out
            return 0
        lax.fori_loop(0, STEPS, body, 0)

    def g_copies(blk, i, slot):
        es = pl.ds(i * Q, Q)
        return [pltpu.make_async_copy(dab_v.at[slot], dab_o.at[blk, es], g_sem.at[slot, 0]),
                pltpu.make_async_copy(mid_v.at[slot], mid_o.at[blk, es], g_sem.at[slot, 1])]

    def experts_bwd(blk, zsrc, rsrc, dst):
        def body(i, _):
            slot, spare = w_next(blk, i), lax.rem(i, 2)

            @pl.when(i >= 2)
            def _():
                for c in g_copies(blk, i - 2, spare):
                    c.wait()
            es = [i * Q + n for n in range(Q)]
            gus = [dot(slots[zsrc, e], wgu[slot, n]) for n, e in enumerate(es)]
            dms = [dot_nt(slots[rsrc, e], wd[slot, n]) for n, e in enumerate(es)]
            dabs = []
            for n in range(Q):
                a, b, dm = gus[n][:, :F], gus[n][:, F:], dms[n]
                sig = jax.nn.sigmoid(a)
                act = a * sig
                mid_v[spare, n] = (act * b).astype(BF16)
                da = (dm * b * (sig * (1.0 + a * (1.0 - sig)))).astype(BF16)
                dabs.append(jnp.concatenate([da, (dm * act).astype(BF16)], axis=1))
            outs = [dot_nt(dab, wgu[slot, n]).astype(BF16) for n, dab in enumerate(dabs)]
            for n, e in enumerate(es):
                dab_v[spare, n] = dabs[n]
                slots[dst, e] = outs[n]
            for c in g_copies(blk, i, spare):
                c.start()
            return 0
        lax.fori_loop(0, STEPS, body, 0)
        for i in (STEPS - 2, STEPS - 1):
            for c in g_copies(blk, i, i % 2):
                c.wait()

    def combine(rs, ch, rt, src, gated):
        def rows_of(s):
            vals = slots[src, :, pl.ds(pl.multiple_of(s * C, C), C), :].reshape(S, D)
            want = lax.broadcasted_iota(I32, (T, 128), 0).astype(F32) + 1.0
            parts = []
            for j in range(NJ):
                val = tb[rt, s, 1, j:j + 1, :] if gated else 1.0
                parts.append(jnp.where(want == tb[rt, s, 0, j:j + 1, :], val, 0.0).astype(BF16))
            return dot(jnp.concatenate(parts, axis=1), vals)

        def sib_copy(q, n):
            return rcopy(part.at[n], sib_in.at[ch, q], sb_s.at[rs, q], sb_r.at[rs, q], dev(1))

        def body(m, _):
            first, last = 1 - lax.div(m + 6, 7), lax.div(m, 7)
            sib = lax.rem(m, 2) + first - last
            n = sib * lax.div(m + 1, 2) + (1 - sib) * (lax.div(m, 2) - 1 + last)
            q, spare = 3 - n, lax.rem(n, 2)

            @pl.when((sib == 1) & (n >= 2))
            def _():
                sib_copy(q + 2, spare).wait_send()
            part[sib * spare + (1 - sib) * 2] = rows_of(peer(2 * q + sib))

            @pl.when(sib == 1)
            def _():
                sib_copy(q, spare).start()

            @pl.when(sib == 0)
            def _():
                sib_copy(q, spare).wait_recv()
                sib_in[ch, q] += part[2]

            @pl.when(m == 2)
            def _():
                for c in tree(rs, ch):
                    c.start()

            @pl.when(m == 4)
            def _():
                fin(rs, ch, 1, 1).start()

            @pl.when(m == 6)
            def _():
                fin(rs, ch, 0, 0).start()
            return 0
        lax.fori_loop(0, 8, body, 0)
        for n in (2, 3):
            sib_copy(3 - n, n % 2).wait_send()

    def rs_mid(rs, ch):
        first, second = tree(rs, ch)
        first.wait()
        sib_in[ch, P_Y, :HALF] += tree_in[ch, LOW]
        fin(rs, ch, 1, 0).start()
        second.wait()
        sib_in[ch, P_X, HALF:] += tree_in[ch, UP]
        fin(rs, ch, 0, 1).start()

    P_OWN, P_X, P_Y, P_DIAG = range(4)

    def tree(rs, ch):
        return [rcopy(sib_in.at[ch, P_DIAG, pl.ds(h * HALF, HALF)], tree_in.at[ch, h], tr_s.at[rs, h], tr_r.at[rs, h], dev(to))
                for h, to in ((LOW, XN), (UP, YN))]

    def fin(rs, ch, axis, half):
        rows = pl.ds(half * HALF, HALF)
        return rcopy(sib_in.at[ch, P_X + axis, rows], fin_in.at[ch, axis, rows], fi_s.at[rs, axis, half], fi_r.at[rs, axis, half], dev(2 + 2 * axis))

    def rs_wait(rs, ch):
        for axis in range(2):
            for half in range(2):
                fin(rs, ch, axis, half).wait()

    def total_of(ch):
        return lambda rows: sib_in[ch, P_OWN, rows, :] + fin_in[ch, 0, rows, :] + fin_in[ch, 1, rows, :]

    def block_out(ch, h_ref, out_ref):
        total = total_of(ch)

        def body(i, _):
            rows = pl.ds(pl.multiple_of(i * ROWS, ROWS), ROWS)
            out_ref[rows, :] = (h_ref[rows, :].astype(F32) + total(rows)).astype(BF16)
            return 0
        lax.fori_loop(0, T // ROWS, body, 0)

    def save(n, slot_array, out, blk):
        return pltpu.make_async_copy(slots.at[slot_array], out.at[blk], l_sem.at[n])

    A_ZB1, A_ZF1, A_G2, A_ZB2, A_ZF2, A_G1 = range(6)
    R_B1, R_F1, R_DB2, R_F2, R_DB1 = range(5)
    w_first(LOW)
    build_tables(B1, FW1)
    pl.semaphore_wait(barrier, G)
    tables_send(B1)
    dense_fwd(LOW, xv.at[XB], hv.at[HB1], zall.at[ZB, me])
    ag_send(A_ZB1, ZB)
    build_tables(FW1, B2)
    tables_send(FW1)
    load_xf.wait()
    dense_fwd(LOW, xv.at[XF], hv.at[HF], zall.at[ZF, me])
    ag_mid(A_ZB1, ZB)
    ag_send(A_ZF1, ZF)
    build_tables(B2, FW2 + 1)
    tables_send(B2)
    tables_send(FW2)

    tables_wait(B1)
    dispatch(A_ZB1, ZB, B1, SB, False)
    save_z1 = save(0, SB, z_o, 0)
    save_z1.start()
    ag_mid(A_ZF1, ZF)
    load_g.wait()
    ag_send(A_G2, GB)
    experts_fwd(LOW, SB, RO)
    w_first(LOW)
    combine(R_B1, BB, B1, RO, True)

    tables_wait(FW1)
    dispatch(A_ZF1, ZF, FW1, SF, False)
    ag_mid(A_G2, GB)
    rs_mid(R_B1, BB)
    experts_fwd(LOW, SF, SF)
    w_first(UP)
    rs_wait(R_B1, BB)
    block_out(BB, hv.at[HB1], xv.at[XB2])
    dense_fwd(UP, xv.at[XB2], hv.at[HB2], zall.at[ZB, me])
    ag_send(A_ZB2, ZB)
    combine(R_F1, FB, FW1, SF, True)
    tables_wait(B2)
    dispatch(A_G2, GB, B2, RO, True)
    save_r2 = save(1, RO, r_o, 1)
    save_r2.start()
    ag_mid(A_ZB2, ZB)
    rs_mid(R_F1, FB)
    save_z1.wait()
    dispatch(A_ZB2, ZB, B2, SB, False)
    save_z2 = save(2, SB, z_o, 1)
    save_z2.start()
    save_r2.wait()
    experts_bwd(UP, SB, RO, RO)
    w_first(UP)
    save_z2.wait()
    load = pltpu.make_async_copy(z_o.at[LOW], slots.at[SB], l_sem.at[3])
    load.start()
    combine(R_DB2, BB, B2, RO, False)

    rs_wait(R_F1, FB)
    block_out(FB, hv.at[HF], xv.at[XF])
    dense_fwd(UP, xv.at[XF], hv.at[HF], zall.at[ZF, me])
    rs_mid(R_DB2, BB)
    ag_send(A_ZF2, ZF)
    rs_wait(R_DB2, BB)
    dense_bwd(UP, xv.at[XB2], hv.at[HB2], zall.at[GB, me], total_of(BB), zall.at[ZB, me])
    ag_mid(A_ZF2, ZF)
    ag_send(A_G1, ZB)
    tables_wait(FW2)
    dispatch(A_ZF2, ZF, FW2, SF, False)
    experts_fwd(UP, SF, SF)
    w_first(LOW)
    ag_mid(A_G1, ZB)
    combine(R_F2, FB, FW2, SF, True)

    dispatch(A_G1, ZB, B1, RO, True)
    save_r1 = save(1, RO, r_o, 0)
    save_r1.start()
    load.wait()
    rs_mid(R_F2, FB)
    experts_bwd(LOW, SB, RO, SB)
    combine(R_DB1, BB, B1, SB, False)
    rs_wait(R_F2, FB)
    block_out(FB, hv.at[HF], yv.at[LOW])
    send_y = rcopy(yv.at[LOW], y_o, o_s.at[LOW], o_r.at[LOW], stage_peer)
    send_y.start()
    rs_mid(R_DB1, BB)
    save_r1.wait()
    rs_wait(R_DB1, BB)
    dense_bwd(LOW, xv.at[XB], hv.at[HB1], zall.at[ZB, me], total_of(BB), yv.at[UP])
    send_x = rcopy(yv.at[UP], dx_o, o_s.at[UP], o_r.at[UP], stage_peer)
    send_x.start()
    send_y.wait()
    send_x.wait()


def weight_grads(z_ref, r_ref, dab_ref, mid_ref, gg_ref, gu_ref, gd_ref):
    for n in range(z_ref.shape[1]):
        dw = dot_tn(z_ref[0, n], dab_ref[0, n])
        gg_ref[0, 0, n] = dw[:, :F]
        gu_ref[0, 0, n] = dw[:, F:]
        gd_ref[0, 0, n] = dot_tn(mid_ref[0, n], r_ref[0, n])


def solution(mesh):
    def local_step(*args):
        arrays = [v[0] for v in args]
        route_fwd, gate_fwd, route_bwd, gate_bwd = arrays[8:]
        route = jnp.stack([v[blk] for blk in range(2) for v in (route_bwd, route_fwd)]).transpose(0, 2, 1)
        gate = jnp.stack([v[blk] for blk in range(2) for v in (gate_bwd, gate_fwd)]).astype(F32).transpose(0, 2, 1)
        vmem, hbm = pl.BlockSpec(memory_space=pltpu.VMEM), pl.BlockSpec(memory_space=pl.ANY)
        dma = pltpu.SemaphoreType.DMA
        tok = jax.ShapeDtypeStruct((T, D), BF16)
        wide = jax.ShapeDtypeStruct((2, E, G * C, D), BF16)
        table = (4, G, 2, 16, 128)
        scratch = [(BF16, [(3, G, T, D), (3, E, G * C, D)]), (F32, [table, table]),
                   (BF16, [(2, D, FF), (2, FF, D), (3, T, D), (3, T, D), (2, T, D)]),
                   (F32, [(3, T, D), (2, 4, T, D), (2, 2, HALF, D), (2, 2, T, D)]),
                   (BF16, [(AHEAD + 1, Q, D, 2 * F), (AHEAD + 1, Q, F, D), (2, Q, G * C, D), (2, Q, G * C, F)])]
        gather, tables, sib, tree, last = (6, 10), (4, G), (5, 4), (5, 2), (5, 2, 2)
        sems = [gather, gather, tables, tables, sib, sib, tree, tree, last, last, (AHEAD + 1, 3), (2, 2), (5,), (2,), (2,)]
        outs = pl.pallas_call(
            kernel,
            out_shape=(tok, tok, wide, wide, wide, jax.ShapeDtypeStruct((2, E, G * C, F), BF16)),
            in_specs=[hbm] * 8 + [vmem] * 2,
            out_specs=(vmem, vmem, hbm, hbm, hbm, hbm),
            scratch_shapes=[pltpu.VMEM(shape, dtype) for dtype, shapes in scratch for shape in shapes] + [dma(shape) for shape in sems],
            compiler_params=pltpu.CompilerParams(collective_id=0, has_side_effects=True, vmem_limit_bytes=67043328),
        )(*arrays[:8], route, gate)
        y_next, dx_prev, z, r, dab, mid = outs
        q = 12
        rows = [pl.BlockSpec((1, q, G * C, w), lambda b, i: (b, i, 0, 0)) for w in (D, D, D, F)]
        up = jax.ShapeDtypeStruct((1, 2, E, D, F), F32)
        down = jax.ShapeDtypeStruct((1, 2, E, F, D), F32)
        up_spec = pl.BlockSpec((1, 1, q, D, F), lambda b, i: (0, b, i, 0, 0))
        down_spec = pl.BlockSpec((1, 1, q, F, D), lambda b, i: (0, b, i, 0, 0))
        dgate, dup, ddown = pl.pallas_call(
            weight_grads,
            grid=(2, E // q),
            out_shape=(up, up, down),
            in_specs=rows,
            out_specs=(up_spec, up_spec, down_spec),
        )(z, r, dab, mid)
        return y_next[None], dx_prev[None], dgate, dup, ddown

    tok_spec = P('pp', 'ep', None)
    dense_spec = P('pp', None, None, None)
    exp_spec = P('pp', None, 'ep', None, None)
    route_spec = P('pp', None, 'ep', None)
    return jax.shard_map(local_step, mesh=mesh, in_specs=(tok_spec, tok_spec, tok_spec, dense_spec, dense_spec, exp_spec, exp_spec, exp_spec, route_spec, route_spec, route_spec, route_spec), out_specs=(tok_spec, tok_spec, exp_spec, exp_spec, exp_spec), check_vma=False)
```

```python
import jax
import jax.numpy as jnp
from jax import lax
from jax.experimental import pallas as pl
from jax.experimental.pallas import tpu as pltpu
from jax.sharding import PartitionSpec as P

MESH = pl.DeviceIdType.MESH
EPS = 1e-6
F32, BF16, I32 = jnp.float32, jnp.bfloat16, jnp.int32
T, D, FF, K = 768, 256, 1024, 8
G, E, C, F = 8, 48, 32, 128
S = E * C
NJ = S // 128
HALF = T // 2
ROWS = 256
B1, FW1, B2, FW2 = range(4)
SIB, XN, YN, DIAG = 1, 2, 4, 6
LOW, UP = 0, 1
BB, FB = 0, 1
Q, AHEAD = 8, 2
STEPS = E // Q


def dot(a, b):
    return jnp.dot(a, b, preferred_element_type=F32)


def dot_nt(a, b):
    return lax.dot_general(a, b, (((1,), (1,)), ((), ())), preferred_element_type=F32)


def dot_tn(a, b):
    return lax.dot_general(a, b, (((0,), (0,)), ((), ())), preferred_element_type=F32)


def rms_norm(v):
    return v * lax.rsqrt(jnp.mean(v * v, axis=-1, keepdims=True) + EPS)


def rms_back(v, g):
    inv = lax.rsqrt(jnp.mean(v * v, axis=-1, keepdims=True) + EPS)
    proj = jnp.mean(g * v, axis=-1, keepdims=True)
    return inv * g - v * (inv * inv * inv) * proj


def xor1(a, b):
    return a + b - 2 * a * b


def kernel(xf_h, xb_h, gin_h, win_h, wout_h, eg_h, eu_h, ed_h, rb_v, rf_v, gb_v, gf_v,
           y_o, dx_o, z_o, r_o, dab_o, mid_o,
           zall, slots, trow, tb, w1, w2, xv, hv, yv,
           part, sib_in, tree_in, fin_in, wgu, wd, dab_v, mid_v,
           ag_s, ag_r, tb_s, tb_r, sb_s, sb_r, tr_s, tr_r, fi_s, fi_r,
           w_sem, g_sem, l_sem, o_s, o_r):
    pp, me = lax.axis_index("pp"), lax.axis_index("ep")
    my_y, my_x, my_c = lax.div(me, 4), lax.rem(lax.div(me, 2), 2), lax.rem(me, 2)
    ZB, ZF, GB = range(3)
    SB, SF, RO = range(3)
    XB, XF, XB2 = range(3)
    HB1, HF, HB2 = range(3)

    def peer(r):
        if isinstance(r, int):
            ry, rx, rc = r // 4, r // 2 % 2, r % 2
        else:
            ry, rx, rc = lax.div(r, 4), lax.rem(lax.div(r, 2), 2), lax.rem(r, 2)
        return xor1(my_y, ry) * 4 + xor1(my_x, rx) * 2 + xor1(my_c, rc)

    def dev(r):
        return {"pp": pp, "ep": peer(r)}

    def rcopy(src, dst, s_sem, r_sem, to):
        return pltpu.make_async_remote_copy(src_ref=src, dst_ref=dst, send_sem=s_sem, recv_sem=r_sem, device_id=to, device_id_type=MESH)

    barrier = pltpu.get_barrier_semaphore()
    for r in range(1, G):
        pl.semaphore_signal(barrier, inc=1, device_id=dev(r), device_id_type=MESH)
    stage_peer = {"pp": 1 - pp, "ep": me}
    pl.semaphore_signal(barrier, inc=1, device_id=stage_peer, device_id_type=MESH)

    pairs = [(gin_h, zall.at[GB, me]), (xb_h, xv.at[XB]), (win_h, w1), (wout_h, w2), (xf_h, xv.at[XF])]
    local = [pltpu.make_async_copy(src, dst, l_sem.at[n]) for n, (src, dst) in enumerate(pairs)]
    for c in local:
        c.start()
    load_g, load_xb, load_w1, load_w2, load_xf = local

    def half(buf, r, h):
        return zall.at[buf, me if r is None else peer(r), pl.ds(h * HALF, HALF)]

    def ag_copy(i, n, ref, r):
        return rcopy(ref, ref, ag_s.at[i, n], ag_r.at[i, n], dev(r))

    X_LOW, X_UP, Y_LOW, Y_UP, OWN, D_LOW, D_UP, PASS = range(8)

    def ag_own(i, buf):
        low, up = half(buf, None, LOW), half(buf, None, UP)
        return [ag_copy(i, X_LOW, low, XN), ag_copy(i, Y_UP, up, YN), ag_copy(i, X_UP, up, XN), ag_copy(i, Y_LOW, low, YN),
                ag_copy(i, OWN, zall.at[buf, me], SIB)]

    def ag_pass(i, buf):
        return ag_copy(i, D_LOW, half(buf, XN, LOW), YN), ag_copy(i, D_UP, half(buf, YN, UP), XN)

    def ag_sib(i, buf, n):
        return ag_copy(i, PASS + n, zall.at[buf, peer((XN, YN, DIAG)[n])], SIB)

    def ag_send(i, buf, parts=slice(None)):
        for c in ag_own(i, buf)[parts]:
            c.start()

    def ag_mid(i, buf):
        first, second = ag_pass(i, buf)
        ag_copy(i, X_LOW, half(buf, XN, LOW), XN).wait_recv()
        first.start()
        ag_copy(i, Y_UP, half(buf, YN, UP), YN).wait_recv()
        second.start()

    def ag_step(i, buf, r):
        waits = [[(OWN, zall.at[buf, peer(SIB)]), (X_UP, half(buf, XN, UP))],
                 [(PASS, zall.at[buf, peer(XN + SIB)]), (Y_LOW, half(buf, YN, LOW))],
                 [(PASS + 1, zall.at[buf, peer(YN + SIB)]), (D_LOW, half(buf, DIAG, LOW)), (D_UP, half(buf, DIAG, UP))],
                 [(PASS + 2, zall.at[buf, peer(DIAG + SIB)])]]
        for n, group in enumerate(waits):
            @pl.when(r == 2 * n + 1)
            def _(n=n, group=group):
                for sem, ref in group:
                    ag_copy(i, sem, ref, SIB).wait_recv()
                if len(group) > 1:
                    ag_sib(i, buf, n).start()

    def ag_finish(i, buf):
        for c in ag_own(i, buf) + list(ag_pass(i, buf)):
            c.wait_send()
        for n in range(3):
            ag_sib(i, buf, n).wait_send()

    def dense_fwd(blk, x_ref, h_ref, z_ref):
        def body(i, _):
            rows = pl.ds(pl.multiple_of(i * ROWS, ROWS), ROWS)
            x = x_ref[rows, :].astype(F32)
            pre = dot(rms_norm(x).astype(BF16), w1[blk])
            h = (x + dot(jax.nn.silu(pre).astype(BF16), w2[blk])).astype(BF16)
            h_ref[rows, :] = h
            z_ref[rows, :] = rms_norm(h.astype(F32)).astype(BF16)
            return 0
        lax.fori_loop(0, T // ROWS, body, 0)

    def silu_grad(a):
        sig = jax.nn.sigmoid(a)
        return sig * (1.0 + a * (1.0 - sig))

    def dense_bwd(blk, x_ref, h_ref, g_ref, total, out_ref, after=None):
        def body(i, _):
            rows = pl.ds(pl.multiple_of(i * ROWS, ROWS), ROWS)
            x = x_ref[rows, :].astype(F32)
            pre = dot(rms_norm(x).astype(BF16), w1[blk])
            dh = g_ref[rows, :].astype(F32) + rms_back(h_ref[rows, :].astype(F32), total(rows))
            dm = dot_nt(dh.astype(BF16), w2[blk])
            dp = (dm * silu_grad(pre)).astype(BF16)
            out_ref[rows, :] = (dh + rms_back(x, dot_nt(dp, w1[blk]))).astype(BF16)
            if after is not None:
                after(i, rows).start()
            return 0
        lax.fori_loop(0, T // ROWS, body, 0)

    def build_tables(ch, blk):
        rt = ch + 2 * blk
        route_ref, gate_ref = ((rb_v, gb_v), (rf_v, gf_v))[ch]

        def body(_, carry):
            acc_i = jnp.zeros((128, 128), F32)
            acc_g = jnp.zeros((128, 128), F32)
            for tc in range(T // 256):
                rows = route_ref[blk, :, tc * 256:(tc + 1) * 256]
                gates = gate_ref[blk, :, tc * 256:(tc + 1) * 256].astype(F32)
                cols, gcols = rows.T, gates.T
                quad = lax.shift_right_logical(rows, 7)
                place = quad + 4 * lax.shift_right_logical(quad * 43, 9)
                lane = lax.bitwise_and(cols, 127)
                tok = lax.broadcasted_iota(I32, (256, 128), 0) + (tc * 256 + 1)
                low = lax.bitwise_and(tok, 255)
                high = (tok - low).astype(F32)
                low = low.astype(F32)
                lanes = lax.broadcasted_iota(I32, (256, 128), 1)
                spots = lax.broadcasted_iota(I32, (128, 256), 0)
                for k in range(K):
                    a = jnp.where(spots == place[k:k + 1, :], 1.0, 0.0).astype(BF16)
                    hit = lanes == lane[:, k:k + 1]
                    b = jnp.concatenate([jnp.where(hit, low, 0.0), jnp.where(hit, high, 0.0)], axis=1).astype(BF16)
                    both = dot(a, b)
                    acc_i += both[:, :128] + both[:, 128:]
                    acc_g += dot(a, jnp.where(hit, gcols[:, k:k + 1], 0.0).astype(BF16))
            trow[rt, :, 0] = acc_i.reshape(G, 16, 128)
            trow[rt, :, 1] = acc_g.reshape(G, 16, 128)
            tb[rt, me] = trow[rt, me]
            return carry
        lax.fori_loop(0, 1, body, 0)

    def tables_send(rt):
        for r in range(1, G):
            rcopy(trow.at[rt, peer(r)], tb.at[rt, me], tb_s.at[rt, r], tb_r.at[rt, r], dev(r)).start()

    def tables_wait(rt):
        for r in range(1, G):
            rcopy(trow.at[rt, peer(r)], tb.at[rt, peer(r)], tb_s.at[rt, r], tb_r.at[rt, r], dev(r)).wait()

    def dispatch(ag, buf, rt, dst, gated):
        def body(r, _):
            if ag is not None:
                ag_step(ag, buf, r)
            src = peer(r)
            z = zall[buf, src]
            cols = tb[rt, src, 0].T
            gcols = tb[rt, src, 1].T if gated else None
            base = pl.multiple_of(src * C, C)
            want = lax.broadcasted_iota(I32, (128, T), 1).astype(F32) + 1.0
            for j in range(0, NJ, 4):
                parts = []
                for q in range(j, j + 4):
                    val = gcols[:, q:q + 1] if gated else 1.0
                    parts.append(jnp.where(want == cols[:, q:q + 1], val, 0.0).astype(BF16))
                got = dot(jnp.concatenate(parts, axis=0), z).astype(BF16)
                slots[dst, 4 * j:4 * j + 16, pl.ds(base, C), :] = got.reshape(16, C, D)
            return 0
        lax.fori_loop(0, G, body, 0)
        if ag is not None:
            ag_finish(ag, buf)

    def w_copies(blk, i):
        slot = i % (AHEAD + 1) if isinstance(i, int) else lax.rem(i, AHEAD + 1)
        es = pl.ds(i * Q, Q)
        return [pltpu.make_async_copy(eg_h.at[blk, es], wgu.at[slot, :, :, pl.ds(0, F)], w_sem.at[slot, 0]),
                pltpu.make_async_copy(eu_h.at[blk, es], wgu.at[slot, :, :, pl.ds(F, F)], w_sem.at[slot, 1]),
                pltpu.make_async_copy(ed_h.at[blk, es], wd.at[slot], w_sem.at[slot, 2])]

    def w_first(blk):
        for i in range(AHEAD):
            for c in w_copies(blk, i):
                c.start()

    def w_next(blk, i):
        @pl.when(i + AHEAD < STEPS)
        def _():
            for c in w_copies(blk, i + AHEAD):
                c.start()
        for c in w_copies(blk, i):
            c.wait()
        return lax.rem(i, AHEAD + 1)

    def experts_fwd(blk, src, dst):
        def body(i, _):
            slot = w_next(blk, i)
            es = [i * Q + n for n in range(Q)]
            gus = [dot(slots[src, e], wgu[slot, n]) for n, e in enumerate(es)]
            mids = [(jax.nn.silu(gu[:, :F]) * gu[:, F:]).astype(BF16) for gu in gus]
            outs = [dot(mid, wd[slot, n]).astype(BF16) for n, mid in enumerate(mids)]
            for e, out in zip(es, outs):
                slots[dst, e] = out
            return 0
        lax.fori_loop(0, STEPS, body, 0)

    def g_copies(blk, i, slot):
        es = pl.ds(i * Q, Q)
        return [pltpu.make_async_copy(dab_v.at[slot], dab_o.at[blk, es], g_sem.at[slot, 0]),
                pltpu.make_async_copy(mid_v.at[slot], mid_o.at[blk, es], g_sem.at[slot, 1])]

    def experts_bwd(blk, zsrc, rsrc, dst):
        def body(i, _):
            slot, spare = w_next(blk, i), lax.rem(i, 2)

            @pl.when(i >= 2)
            def _():
                for c in g_copies(blk, i - 2, spare):
                    c.wait()
            es = [i * Q + n for n in range(Q)]
            gus = [dot(slots[zsrc, e], wgu[slot, n]) for n, e in enumerate(es)]
            dms = [dot_nt(slots[rsrc, e], wd[slot, n]) for n, e in enumerate(es)]
            dabs = []
            for n in range(Q):
                a, b, dm = gus[n][:, :F], gus[n][:, F:], dms[n]
                sig = jax.nn.sigmoid(a)
                act = a * sig
                mid_v[spare, n] = (act * b).astype(BF16)
                da = (dm * b * (sig * (1.0 + a * (1.0 - sig)))).astype(BF16)
                dabs.append(jnp.concatenate([da, (dm * act).astype(BF16)], axis=1))
            outs = [dot_nt(dab, wgu[slot, n]).astype(BF16) for n, dab in enumerate(dabs)]
            for n, e in enumerate(es):
                dab_v[spare, n] = dabs[n]
                slots[dst, e] = outs[n]
            for c in g_copies(blk, i, spare):
                c.start()
            return 0
        lax.fori_loop(0, STEPS, body, 0)
        for i in (STEPS - 2, STEPS - 1):
            for c in g_copies(blk, i, i % 2):
                c.wait()

    def combine(rs, ch, rt, src, gated):
        def rows_of(s):
            vals = slots[src, :, pl.ds(pl.multiple_of(s * C, C), C), :].reshape(S, D)
            want = lax.broadcasted_iota(I32, (T, 128), 0).astype(F32) + 1.0
            parts = []
            for j in range(NJ):
                val = tb[rt, s, 1, j:j + 1, :] if gated else 1.0
                parts.append(jnp.where(want == tb[rt, s, 0, j:j + 1, :], val, 0.0).astype(BF16))
            return dot(jnp.concatenate(parts, axis=1), vals)

        def sib_copy(q, n):
            return rcopy(part.at[n], sib_in.at[ch, q], sb_s.at[rs, q], sb_r.at[rs, q], dev(1))

        def body(m, _):
            first, last = 1 - lax.div(m + 6, 7), lax.div(m, 7)
            sib = lax.rem(m, 2) + first - last
            n = sib * lax.div(m + 1, 2) + (1 - sib) * (lax.div(m, 2) - 1 + last)
            q, spare = 3 - n, lax.rem(n, 2)

            @pl.when((sib == 1) & (n >= 2))
            def _():
                sib_copy(q + 2, spare).wait_send()
            part[sib * spare + (1 - sib) * 2] = rows_of(peer(2 * q + sib))

            @pl.when(sib == 1)
            def _():
                sib_copy(q, spare).start()

            @pl.when(sib == 0)
            def _():
                sib_copy(q, spare).wait_recv()
                sib_in[ch, q] += part[2]

            @pl.when(m == 2)
            def _():
                for c in tree(rs, ch):
                    c.start()

            @pl.when(m == 4)
            def _():
                fin(rs, ch, 1, 1).start()

            @pl.when(m == 6)
            def _():
                fin(rs, ch, 0, 0).start()
            return 0
        lax.fori_loop(0, 8, body, 0)
        for n in (2, 3):
            sib_copy(3 - n, n % 2).wait_send()

    def rs_mid(rs, ch):
        first, second = tree(rs, ch)
        first.wait()
        sib_in[ch, P_Y, :HALF] += tree_in[ch, LOW]
        fin(rs, ch, 1, 0).start()
        second.wait()
        sib_in[ch, P_X, HALF:] += tree_in[ch, UP]
        fin(rs, ch, 0, 1).start()

    P_OWN, P_X, P_Y, P_DIAG = range(4)

    def tree(rs, ch):
        return [rcopy(sib_in.at[ch, P_DIAG, pl.ds(h * HALF, HALF)], tree_in.at[ch, h], tr_s.at[rs, h], tr_r.at[rs, h], dev(to))
                for h, to in ((LOW, XN), (UP, YN))]

    def fin(rs, ch, axis, half):
        rows = pl.ds(half * HALF, HALF)
        return rcopy(sib_in.at[ch, P_X + axis, rows], fin_in.at[ch, axis, rows], fi_s.at[rs, axis, half], fi_r.at[rs, axis, half], dev(2 + 2 * axis))

    def rs_wait(rs, ch):
        for axis in range(2):
            for half in range(2):
                fin(rs, ch, axis, half).wait()

    def total_of(ch):
        return lambda rows: sib_in[ch, P_OWN, rows, :] + fin_in[ch, 0, rows, :] + fin_in[ch, 1, rows, :]

    def block_out(ch, h_ref, out_ref):
        total = total_of(ch)

        def body(i, _):
            rows = pl.ds(pl.multiple_of(i * ROWS, ROWS), ROWS)
            out_ref[rows, :] = (h_ref[rows, :].astype(F32) + total(rows)).astype(BF16)
            return 0
        lax.fori_loop(0, T // ROWS, body, 0)

    def save(n, slot_array, out, blk):
        return pltpu.make_async_copy(slots.at[slot_array], out.at[blk], l_sem.at[n])

    A_ZB1, A_ZF1, A_G2, A_ZB2, A_ZF2, A_G1 = range(6)
    R_B1, R_F1, R_DB2, R_F2, R_DB1 = range(5)
    build_tables(BB, LOW)
    load_g.wait()
    pl.semaphore_wait(barrier, G)
    tables_send(B1)
    ag_send(A_G2, GB, slice(2))
    w_first(LOW)
    for c in (load_xb, load_w1, load_w2):
        c.wait()
    dense_fwd(LOW, xv.at[XB], hv.at[HB1], zall.at[ZB, me])
    ag_send(A_ZB1, ZB)
    build_tables(FB, LOW)
    tables_send(FW1)
    load_xf.wait()
    dense_fwd(LOW, xv.at[XF], hv.at[HF], zall.at[ZF, me])
    ag_mid(A_ZB1, ZB)
    ag_send(A_ZF1, ZF)
    build_tables(BB, UP)
    build_tables(FB, UP)
    tables_send(B2)
    tables_send(FW2)

    tables_wait(B1)
    dispatch(A_ZB1, ZB, B1, SB, False)
    save_z1 = save(0, SB, z_o, 0)
    save_z1.start()
    ag_mid(A_ZF1, ZF)
    ag_send(A_G2, GB, slice(2, None))
    experts_fwd(LOW, SB, RO)
    w_first(LOW)
    combine(R_B1, BB, B1, RO, True)

    tables_wait(FW1)
    dispatch(A_ZF1, ZF, FW1, SF, False)
    ag_mid(A_G2, GB)
    rs_mid(R_B1, BB)
    experts_fwd(LOW, SF, SF)
    w_first(UP)
    rs_wait(R_B1, BB)
    block_out(BB, hv.at[HB1], xv.at[XB2])
    dense_fwd(UP, xv.at[XB2], hv.at[HB2], zall.at[ZB, me])
    ag_send(A_ZB2, ZB)
    tables_wait(B2)
    dispatch(A_G2, GB, B2, RO, True)
    save_r2 = save(1, RO, r_o, 1)
    save_r2.start()
    ag_mid(A_ZB2, ZB)
    combine(R_F1, FB, FW1, SF, True)
    save_z1.wait()
    dispatch(A_ZB2, ZB, B2, SB, False)
    rs_mid(R_F1, FB)
    save_z2 = save(2, SB, z_o, 1)
    save_z2.start()
    save_r2.wait()
    experts_bwd(UP, SB, RO, RO)
    w_first(UP)
    save_z2.wait()
    load = pltpu.make_async_copy(z_o.at[LOW], slots.at[SB], l_sem.at[3])
    load.start()
    combine(R_DB2, BB, B2, RO, False)

    rs_wait(R_F1, FB)
    block_out(FB, hv.at[HF], xv.at[XF])
    dense_fwd(UP, xv.at[XF], hv.at[HF], zall.at[ZF, me])
    rs_mid(R_DB2, BB)
    ag_send(A_ZF2, ZF)
    rs_wait(R_DB2, BB)
    dense_bwd(UP, xv.at[XB2], hv.at[HB2], zall.at[GB, me], total_of(BB), zall.at[ZB, me])
    ag_mid(A_ZF2, ZF)
    ag_send(A_G1, ZB)
    tables_wait(FW2)
    dispatch(A_ZF2, ZF, FW2, SF, False)
    experts_fwd(UP, SF, SF)
    w_first(LOW)
    ag_mid(A_G1, ZB)
    combine(R_F2, FB, FW2, SF, True)

    dispatch(A_G1, ZB, B1, RO, True)
    save_r1 = save(1, RO, r_o, 0)
    save_r1.start()
    load.wait()
    rs_mid(R_F2, FB)
    experts_bwd(LOW, SB, RO, SB)
    combine(R_DB1, BB, B1, SB, False)
    rs_wait(R_F2, FB)
    block_out(FB, hv.at[HF], yv.at[LOW])
    send_y = rcopy(yv.at[LOW], y_o, o_s.at[LOW], o_r.at[LOW], stage_peer)
    send_y.start()
    rs_mid(R_DB1, BB)
    save_r1.wait()
    rs_wait(R_DB1, BB)

    def send_x(i, rows):
        return rcopy(yv.at[UP, rows], dx_o.at[rows], o_s.at[1 + i], o_r.at[1 + i], stage_peer)

    dense_bwd(LOW, xv.at[XB], hv.at[HB1], zall.at[ZB, me], total_of(BB), yv.at[UP], send_x)
    send_y.wait()
    for i in range(T // ROWS):
        send_x(i, pl.ds(i * ROWS, ROWS)).wait()


def weight_grads(z_ref, r_ref, dab_ref, mid_ref, gg_ref, gu_ref, gd_ref):
    for n in range(z_ref.shape[1]):
        dw = dot_tn(z_ref[0, n], dab_ref[0, n])
        gg_ref[0, 0, n] = dw[:, :F]
        gu_ref[0, 0, n] = dw[:, F:]
        gd_ref[0, 0, n] = dot_tn(mid_ref[0, n], r_ref[0, n])


def solution(mesh):
    def local_step(*args):
        arrays = [v[0] for v in args]
        route_fwd, gate_fwd, route_bwd, gate_bwd = arrays[8:]
        index = [v.transpose(0, 2, 1) for v in (route_bwd, route_fwd, gate_bwd, gate_fwd)]
        vmem, hbm = pl.BlockSpec(memory_space=pltpu.VMEM), pl.BlockSpec(memory_space=pl.ANY)
        dma = pltpu.SemaphoreType.DMA
        tok = jax.ShapeDtypeStruct((T, D), BF16)
        wide = jax.ShapeDtypeStruct((2, E, G * C, D), BF16)
        table = (4, G, 2, 16, 128)
        scratch = [(BF16, [(3, G, T, D), (3, E, G * C, D)]), (F32, [table, table]),
                   (BF16, [(2, D, FF), (2, FF, D), (3, T, D), (3, T, D), (2, T, D)]),
                   (F32, [(3, T, D), (2, 4, T, D), (2, 2, HALF, D), (2, 2, T, D)]),
                   (BF16, [(AHEAD + 1, Q, D, 2 * F), (AHEAD + 1, Q, F, D), (2, Q, G * C, D), (2, Q, G * C, F)])]
        gather, tables, sib, tree, last = (6, 10), (4, G), (5, 4), (5, 2), (5, 2, 2)
        sems = [gather, gather, tables, tables, sib, sib, tree, tree, last, last, (AHEAD + 1, 3), (2, 2), (5,), (4,), (4,)]
        outs = pl.pallas_call(
            kernel,
            out_shape=(tok, tok, wide, wide, wide, jax.ShapeDtypeStruct((2, E, G * C, F), BF16)),
            in_specs=[hbm] * 8 + [vmem] * 4,
            out_specs=(vmem, vmem, hbm, hbm, hbm, hbm),
            scratch_shapes=[pltpu.VMEM(shape, dtype) for dtype, shapes in scratch for shape in shapes] + [dma(shape) for shape in sems],
            compiler_params=pltpu.CompilerParams(collective_id=0, has_side_effects=True, vmem_limit_bytes=67043328),
        )(*arrays[:8], *index)
        y_next, dx_prev, z, r, dab, mid = outs
        q = 12
        rows = [pl.BlockSpec((1, q, G * C, w), lambda b, i: (b, i, 0, 0)) for w in (D, D, D, F)]
        up = jax.ShapeDtypeStruct((1, 2, E, D, F), F32)
        down = jax.ShapeDtypeStruct((1, 2, E, F, D), F32)
        up_spec = pl.BlockSpec((1, 1, q, D, F), lambda b, i: (0, b, i, 0, 0))
        down_spec = pl.BlockSpec((1, 1, q, F, D), lambda b, i: (0, b, i, 0, 0))
        dgate, dup, ddown = pl.pallas_call(
            weight_grads,
            grid=(2, E // q),
            out_shape=(up, up, down),
            in_specs=rows,
            out_specs=(up_spec, up_spec, down_spec),
        )(z, r, dab, mid)
        return y_next[None], dx_prev[None], dgate, dup, ddown

    tok_spec = P('pp', 'ep', None)
    dense_spec = P('pp', None, None, None)
    exp_spec = P('pp', None, 'ep', None, None)
    route_spec = P('pp', None, 'ep', None)
    return jax.shard_map(local_step, mesh=mesh, in_specs=(tok_spec, tok_spec, tok_spec, dense_spec, dense_spec, exp_spec, exp_spec, exp_spec, route_spec, route_spec, route_spec, route_spec), out_specs=(tok_spec, tok_spec, exp_spec, exp_spec, exp_spec), check_vma=False)
```

```python
import jax
import jax.numpy as jnp
from jax import lax
from jax.experimental import pallas as pl
from jax.experimental.pallas import tpu as pltpu
from jax.sharding import PartitionSpec as P

MESH = pl.DeviceIdType.MESH
EPS = 1e-6
F32, BF16, I32 = jnp.float32, jnp.bfloat16, jnp.int32
T, D, FF, K = 768, 256, 1024, 8
G, E, C, F = 8, 48, 32, 128
S = E * C
NJ = S // 128
HALF = T // 2
PIECE = HALF // 2
ROWS = 256
B1, FW1, B2, FW2 = range(4)
SIB, XN, YN, DIAG = 1, 2, 4, 6
LOW, UP = 0, 1
BB, FB = 0, 1
Q, AHEAD = 8, 2
STEPS = E // Q


def dot(a, b):
    return jnp.dot(a, b, preferred_element_type=F32)


def dot_nt(a, b):
    return lax.dot_general(a, b, (((1,), (1,)), ((), ())), preferred_element_type=F32)


def dot_tn(a, b):
    return lax.dot_general(a, b, (((0,), (0,)), ((), ())), preferred_element_type=F32)


def rms_norm(v):
    return v * lax.rsqrt(jnp.mean(v * v, axis=-1, keepdims=True) + EPS)


def rms_back(v, g):
    inv = lax.rsqrt(jnp.mean(v * v, axis=-1, keepdims=True) + EPS)
    proj = jnp.mean(g * v, axis=-1, keepdims=True)
    return inv * g - v * (inv * inv * inv) * proj


def xor1(a, b):
    return a + b - 2 * a * b


def kernel(xf_h, xb_h, gin_h, win_h, wout_h, eg_h, eu_h, ed_h, rb_v, rf_v, gb_v, gf_v,
           y_o, dx_o, z_o, r_o, dab_o, mid_o,
           zall, slots, trow, tb, w1, w2, xv, hv, yv,
           part, sib_in, tree_in, fin_in, wgu, wd, dab_v, mid_v,
           ag_s, ag_r, tb_s, tb_r, sb_s, sb_r, tr_s, tr_r, fi_s, fi_r,
           w_sem, g_sem, l_sem, o_s, o_r):
    pp, me = lax.axis_index("pp"), lax.axis_index("ep")
    my_y, my_x, my_c = lax.div(me, 4), lax.rem(lax.div(me, 2), 2), lax.rem(me, 2)
    ZB, ZF, GB = range(3)
    SB, SF, RO = range(3)
    XB, XF, XB2 = range(3)
    HB1, HF, HB2 = range(3)

    def peer(r):
        if isinstance(r, int):
            ry, rx, rc = r // 4, r // 2 % 2, r % 2
        else:
            ry, rx, rc = lax.div(r, 4), lax.rem(lax.div(r, 2), 2), lax.rem(r, 2)
        return xor1(my_y, ry) * 4 + xor1(my_x, rx) * 2 + xor1(my_c, rc)

    def dev(r):
        return {"pp": pp, "ep": peer(r)}

    def rcopy(src, dst, s_sem, r_sem, to):
        return pltpu.make_async_remote_copy(src_ref=src, dst_ref=dst, send_sem=s_sem, recv_sem=r_sem, device_id=to, device_id_type=MESH)

    barrier = pltpu.get_barrier_semaphore()
    for r in range(1, G):
        pl.semaphore_signal(barrier, inc=1, device_id=dev(r), device_id_type=MESH)
    stage_peer = {"pp": 1 - pp, "ep": me}
    pl.semaphore_signal(barrier, inc=1, device_id=stage_peer, device_id_type=MESH)

    pairs = [(gin_h, zall.at[GB, me]), (xb_h, xv.at[XB]), (win_h, w1), (wout_h, w2), (xf_h, xv.at[XF])]
    local = [pltpu.make_async_copy(src, dst, l_sem.at[n]) for n, (src, dst) in enumerate(pairs)]
    for c in local:
        c.start()
    load_g, load_xb, load_w1, load_w2, load_xf = local

    def half(buf, r, h):
        return zall.at[buf, me if r is None else peer(r), pl.ds(h * HALF, HALF)]

    def ag_copy(i, n, ref, r):
        return rcopy(ref, ref, ag_s.at[i, n], ag_r.at[i, n], dev(r))

    X_LOW, X_UP, Y_LOW, Y_UP, OWN, D_LOW, D_UP, PASS = range(8)

    def ag_own(i, buf):
        low, up = half(buf, None, LOW), half(buf, None, UP)
        return [ag_copy(i, X_LOW, low, XN), ag_copy(i, Y_UP, up, YN), ag_copy(i, X_UP, up, XN), ag_copy(i, Y_LOW, low, YN),
                ag_copy(i, OWN, zall.at[buf, me], SIB)]

    def ag_pass(i, buf):
        return ag_copy(i, D_LOW, half(buf, XN, LOW), YN), ag_copy(i, D_UP, half(buf, YN, UP), XN)

    def ag_sib(i, buf, n):
        return ag_copy(i, PASS + n, zall.at[buf, peer((XN, YN, DIAG)[n])], SIB)

    def ag_send(i, buf, parts=slice(None)):
        for c in ag_own(i, buf)[parts]:
            c.start()

    def ag_mid(i, buf):
        first, second = ag_pass(i, buf)
        ag_copy(i, X_LOW, half(buf, XN, LOW), XN).wait_recv()
        first.start()
        ag_copy(i, Y_UP, half(buf, YN, UP), YN).wait_recv()
        second.start()

    def ag_step(i, buf, r):
        waits = [[(OWN, zall.at[buf, peer(SIB)]), (X_UP, half(buf, XN, UP))],
                 [(PASS, zall.at[buf, peer(XN + SIB)]), (Y_LOW, half(buf, YN, LOW))],
                 [(PASS + 1, zall.at[buf, peer(YN + SIB)]), (D_LOW, half(buf, DIAG, LOW)), (D_UP, half(buf, DIAG, UP))],
                 [(PASS + 2, zall.at[buf, peer(DIAG + SIB)])]]
        for n, group in enumerate(waits):
            @pl.when(r == 2 * n + 1)
            def _(n=n, group=group):
                for sem, ref in group:
                    ag_copy(i, sem, ref, SIB).wait_recv()
                if len(group) > 1:
                    ag_sib(i, buf, n).start()

    def ag_finish(i, buf):
        for c in ag_own(i, buf) + list(ag_pass(i, buf)):
            c.wait_send()
        for n in range(3):
            ag_sib(i, buf, n).wait_send()

    def dense_fwd(blk, x_ref, h_ref, z_ref):
        def body(i, _):
            rows = pl.ds(pl.multiple_of(i * ROWS, ROWS), ROWS)
            x = x_ref[rows, :].astype(F32)
            pre = dot(rms_norm(x).astype(BF16), w1[blk])
            h = (x + dot(jax.nn.silu(pre).astype(BF16), w2[blk])).astype(BF16)
            h_ref[rows, :] = h
            z_ref[rows, :] = rms_norm(h.astype(F32)).astype(BF16)
            return 0
        lax.fori_loop(0, T // ROWS, body, 0)

    def silu_grad(a):
        sig = jax.nn.sigmoid(a)
        return sig * (1.0 + a * (1.0 - sig))

    def dense_bwd(blk, x_ref, h_ref, g_ref, total, out_ref, before=None, after=None):
        def body(i, _):
            k, h = lax.div(i, 2), lax.rem(i, 2)
            if before is not None:
                @pl.when(h == 0)
                def _():
                    before(k)
            rows = piece(h, k)
            x = x_ref[rows, :].astype(F32)
            pre = dot(rms_norm(x).astype(BF16), w1[blk])
            dh = g_ref[rows, :].astype(F32) + rms_back(h_ref[rows, :].astype(F32), total(rows))
            dm = dot_nt(dh.astype(BF16), w2[blk])
            dp = (dm * silu_grad(pre)).astype(BF16)
            out_ref[rows, :] = (dh + rms_back(x, dot_nt(dp, w1[blk]))).astype(BF16)
            if after is not None:
                after(i, rows).start()
            return 0
        lax.fori_loop(0, 4, body, 0)

    def build_tables(ch, blk):
        rt = ch + 2 * blk
        route_ref, gate_ref = ((rb_v, gb_v), (rf_v, gf_v))[ch]

        def body(_, carry):
            acc_i = jnp.zeros((128, 128), F32)
            acc_g = jnp.zeros((128, 128), F32)
            for tc in range(T // 256):
                rows = route_ref[blk, :, tc * 256:(tc + 1) * 256]
                gates = gate_ref[blk, :, tc * 256:(tc + 1) * 256].astype(F32)
                cols, gcols = rows.T, gates.T
                quad = lax.shift_right_logical(rows, 7)
                place = quad + 4 * lax.shift_right_logical(quad * 43, 9)
                lane = lax.bitwise_and(cols, 127)
                tok = lax.broadcasted_iota(I32, (256, 128), 0) + (tc * 256 + 1)
                low = lax.bitwise_and(tok, 255)
                high = (tok - low).astype(F32)
                low = low.astype(F32)
                lanes = lax.broadcasted_iota(I32, (256, 128), 1)
                spots = lax.broadcasted_iota(I32, (128, 256), 0)
                for k in range(K):
                    a = jnp.where(spots == place[k:k + 1, :], 1.0, 0.0).astype(BF16)
                    hit = lanes == lane[:, k:k + 1]
                    b = jnp.concatenate([jnp.where(hit, low, 0.0), jnp.where(hit, high, 0.0)], axis=1).astype(BF16)
                    both = dot(a, b)
                    acc_i += both[:, :128] + both[:, 128:]
                    acc_g += dot(a, jnp.where(hit, gcols[:, k:k + 1], 0.0).astype(BF16))
            trow[rt, :, 0] = acc_i.reshape(G, 16, 128)
            trow[rt, :, 1] = acc_g.reshape(G, 16, 128)
            tb[rt, me] = trow[rt, me]
            return carry
        lax.fori_loop(0, 1, body, 0)

    def tables_send(rt):
        for r in range(1, G):
            rcopy(trow.at[rt, peer(r)], tb.at[rt, me], tb_s.at[rt, r], tb_r.at[rt, r], dev(r)).start()

    def tables_wait(rt):
        for r in range(1, G):
            rcopy(trow.at[rt, peer(r)], tb.at[rt, peer(r)], tb_s.at[rt, r], tb_r.at[rt, r], dev(r)).wait()

    def dispatch(ag, buf, rt, dst, gated):
        def body(r, _):
            if ag is not None:
                ag_step(ag, buf, r)
            src = peer(r)
            z = zall[buf, src]
            cols = tb[rt, src, 0].T
            gcols = tb[rt, src, 1].T if gated else None
            base = pl.multiple_of(src * C, C)
            want = lax.broadcasted_iota(I32, (128, T), 1).astype(F32) + 1.0
            for j in range(0, NJ, 4):
                parts = []
                for q in range(j, j + 4):
                    val = gcols[:, q:q + 1] if gated else 1.0
                    parts.append(jnp.where(want == cols[:, q:q + 1], val, 0.0).astype(BF16))
                got = dot(jnp.concatenate(parts, axis=0), z).astype(BF16)
                slots[dst, 4 * j:4 * j + 16, pl.ds(base, C), :] = got.reshape(16, C, D)
            return 0
        lax.fori_loop(0, G, body, 0)
        if ag is not None:
            ag_finish(ag, buf)

    def w_copies(blk, i):
        slot = i % (AHEAD + 1) if isinstance(i, int) else lax.rem(i, AHEAD + 1)
        es = pl.ds(i * Q, Q)
        return [pltpu.make_async_copy(eg_h.at[blk, es], wgu.at[slot, :, :, pl.ds(0, F)], w_sem.at[slot, 0]),
                pltpu.make_async_copy(eu_h.at[blk, es], wgu.at[slot, :, :, pl.ds(F, F)], w_sem.at[slot, 1]),
                pltpu.make_async_copy(ed_h.at[blk, es], wd.at[slot], w_sem.at[slot, 2])]

    def w_first(blk):
        for i in range(AHEAD):
            for c in w_copies(blk, i):
                c.start()

    def w_next(blk, i):
        @pl.when(i + AHEAD < STEPS)
        def _():
            for c in w_copies(blk, i + AHEAD):
                c.start()
        for c in w_copies(blk, i):
            c.wait()
        return lax.rem(i, AHEAD + 1)

    def experts_fwd(blk, src, dst):
        def body(i, _):
            slot = w_next(blk, i)
            es = [i * Q + n for n in range(Q)]
            gus = [dot(slots[src, e], wgu[slot, n]) for n, e in enumerate(es)]
            mids = [(jax.nn.silu(gu[:, :F]) * gu[:, F:]).astype(BF16) for gu in gus]
            outs = [dot(mid, wd[slot, n]).astype(BF16) for n, mid in enumerate(mids)]
            for e, out in zip(es, outs):
                slots[dst, e] = out
            return 0
        lax.fori_loop(0, STEPS, body, 0)

    def g_copies(blk, i, slot):
        es = pl.ds(i * Q, Q)
        return [pltpu.make_async_copy(dab_v.at[slot], dab_o.at[blk, es], g_sem.at[slot, 0]),
                pltpu.make_async_copy(mid_v.at[slot], mid_o.at[blk, es], g_sem.at[slot, 1])]

    def experts_bwd(blk, zsrc, rsrc, dst):
        def body(i, _):
            slot, spare = w_next(blk, i), lax.rem(i, 2)

            @pl.when(i >= 2)
            def _():
                for c in g_copies(blk, i - 2, spare):
                    c.wait()
            es = [i * Q + n for n in range(Q)]
            gus = [dot(slots[zsrc, e], wgu[slot, n]) for n, e in enumerate(es)]
            dms = [dot_nt(slots[rsrc, e], wd[slot, n]) for n, e in enumerate(es)]
            dabs = []
            for n in range(Q):
                a, b, dm = gus[n][:, :F], gus[n][:, F:], dms[n]
                sig = jax.nn.sigmoid(a)
                act = a * sig
                mid_v[spare, n] = (act * b).astype(BF16)
                da = (dm * b * (sig * (1.0 + a * (1.0 - sig)))).astype(BF16)
                dabs.append(jnp.concatenate([da, (dm * act).astype(BF16)], axis=1))
            outs = [dot_nt(dab, wgu[slot, n]).astype(BF16) for n, dab in enumerate(dabs)]
            for n, e in enumerate(es):
                dab_v[spare, n] = dabs[n]
                slots[dst, e] = outs[n]
            for c in g_copies(blk, i, spare):
                c.start()
            return 0
        lax.fori_loop(0, STEPS, body, 0)
        for i in (STEPS - 2, STEPS - 1):
            for c in g_copies(blk, i, i % 2):
                c.wait()

    def combine(rs, ch, rt, src, gated, tail=False):
        def rows_of(s):
            vals = slots[src, :, pl.ds(pl.multiple_of(s * C, C), C), :].reshape(S, D)
            want = lax.broadcasted_iota(I32, (T, 128), 0).astype(F32) + 1.0
            parts = []
            for j in range(NJ):
                val = tb[rt, s, 1, j:j + 1, :] if gated else 1.0
                parts.append(jnp.where(want == tb[rt, s, 0, j:j + 1, :], val, 0.0).astype(BF16))
            return dot(jnp.concatenate(parts, axis=1), vals)

        def sib_copy(q, n):
            return rcopy(part.at[n], sib_in.at[ch, q], sb_s.at[rs, q], sb_r.at[rs, q], dev(1))

        def body(m, _):
            first, last = 1 - lax.div(m + 6, 7), lax.div(m, 7)
            sib = lax.rem(m, 2) + first - last
            n = sib * lax.div(m + 1, 2) + (1 - sib) * (lax.div(m, 2) - 1 + last)
            q, spare = 3 - n, lax.rem(n, 2)

            @pl.when((sib == 1) & (n >= 2))
            def _():
                sib_copy(q + 2, spare).wait_send()
            part[sib * spare + (1 - sib) * 2] = rows_of(peer(2 * q + sib))

            @pl.when(sib == 1)
            def _():
                sib_copy(q, spare).start()

            @pl.when(sib == 0)
            def _():
                sib_copy(q, spare).wait_recv()
                sib_in[ch, q] += part[2]

            @pl.when(m == 2)
            def _():
                for k in range(2):
                    for c in tree(rs, ch, k):
                        c.start()

            if not tail:
                for step, axis, h in ((4, 1, UP), (6, 0, LOW)):
                    @pl.when(m == step)
                    def _(axis=axis, h=h):
                        for k in range(2):
                            fin(rs, ch, axis, h, k).start()
            return 0
        lax.fori_loop(0, 8, body, 0)
        for n in (2, 3):
            sib_copy(3 - n, n % 2).wait_send()

    def piece(h, k):
        return pl.ds(pl.multiple_of(h * HALF + k * PIECE, PIECE), PIECE)

    def rs_mid(rs, ch, tail=False):
        for k in range(2):
            for h, c in enumerate(tree(rs, ch, k)):
                c.wait()
                sib_in[ch, P_Y - h, piece(h, k)] += tree_in[ch, h, pl.ds(k * PIECE, PIECE)]
                fin(rs, ch, 1 - h, h, k).start()
            if tail:
                for h in range(2):
                    fin(rs, ch, h, h, k).start()

    P_OWN, P_X, P_Y, P_DIAG = range(4)

    def tree(rs, ch, k):
        return [rcopy(sib_in.at[ch, P_DIAG, piece(h, k)], tree_in.at[ch, h, pl.ds(k * PIECE, PIECE)],
                      tr_s.at[rs, h, k], tr_r.at[rs, h, k], dev(to)) for h, to in ((LOW, XN), (UP, YN))]

    def fin(rs, ch, axis, h, k):
        rows = piece(h, k)
        return rcopy(sib_in.at[ch, P_X + axis, rows], fin_in.at[ch, axis, rows], fi_s.at[rs, axis, h, k], fi_r.at[rs, axis, h, k], dev(2 + 2 * axis))

    def rs_piece(rs, ch, k):
        for axis in range(2):
            for h in range(2):
                fin(rs, ch, axis, h, k).wait()

    def rs_wait(rs, ch):
        for k in range(2):
            rs_piece(rs, ch, k)

    def total_of(ch):
        return lambda rows: sib_in[ch, P_OWN, rows, :] + fin_in[ch, 0, rows, :] + fin_in[ch, 1, rows, :]

    def block_out(ch, h_ref, out_ref):
        total = total_of(ch)

        def body(i, _):
            rows = pl.ds(pl.multiple_of(i * ROWS, ROWS), ROWS)
            out_ref[rows, :] = (h_ref[rows, :].astype(F32) + total(rows)).astype(BF16)
            return 0
        lax.fori_loop(0, T // ROWS, body, 0)

    def save(n, slot_array, out, blk):
        return pltpu.make_async_copy(slots.at[slot_array], out.at[blk], l_sem.at[n])

    A_ZB1, A_ZF1, A_G2, A_ZB2, A_ZF2, A_G1 = range(6)
    R_B1, R_F1, R_DB2, R_F2, R_DB1 = range(5)
    build_tables(BB, LOW)
    load_g.wait()
    pl.semaphore_wait(barrier, G)
    tables_send(B1)
    ag_send(A_G2, GB, slice(2))
    w_first(LOW)
    for c in (load_xb, load_w1, load_w2):
        c.wait()
    dense_fwd(LOW, xv.at[XB], hv.at[HB1], zall.at[ZB, me])
    ag_send(A_ZB1, ZB)
    build_tables(FB, LOW)
    tables_send(FW1)
    load_xf.wait()
    dense_fwd(LOW, xv.at[XF], hv.at[HF], zall.at[ZF, me])
    ag_mid(A_ZB1, ZB)
    ag_send(A_ZF1, ZF)
    build_tables(BB, UP)
    build_tables(FB, UP)
    tables_send(B2)
    tables_send(FW2)

    tables_wait(B1)
    dispatch(A_ZB1, ZB, B1, SB, False)
    save_z1 = save(0, SB, z_o, 0)
    save_z1.start()
    ag_mid(A_ZF1, ZF)
    ag_send(A_G2, GB, slice(2, None))
    experts_fwd(LOW, SB, RO)
    w_first(LOW)
    combine(R_B1, BB, B1, RO, True)

    tables_wait(FW1)
    dispatch(A_ZF1, ZF, FW1, SF, False)
    ag_mid(A_G2, GB)
    rs_mid(R_B1, BB)
    experts_fwd(LOW, SF, SF)
    w_first(UP)
    rs_wait(R_B1, BB)
    block_out(BB, hv.at[HB1], xv.at[XB2])
    dense_fwd(UP, xv.at[XB2], hv.at[HB2], zall.at[ZB, me])
    ag_send(A_ZB2, ZB)
    tables_wait(B2)
    dispatch(A_G2, GB, B2, RO, True)
    save_r2 = save(1, RO, r_o, 1)
    save_r2.start()
    ag_mid(A_ZB2, ZB)
    combine(R_F1, FB, FW1, SF, True)
    save_z1.wait()
    dispatch(A_ZB2, ZB, B2, SB, False)
    rs_mid(R_F1, FB)
    save_z2 = save(2, SB, z_o, 1)
    save_z2.start()
    save_r2.wait()
    experts_bwd(UP, SB, RO, RO)
    w_first(UP)
    save_z2.wait()
    load = pltpu.make_async_copy(z_o.at[LOW], slots.at[SB], l_sem.at[3])
    load.start()
    combine(R_DB2, BB, B2, RO, False)

    rs_wait(R_F1, FB)
    block_out(FB, hv.at[HF], xv.at[XF])
    dense_fwd(UP, xv.at[XF], hv.at[HF], zall.at[ZF, me])
    rs_mid(R_DB2, BB)
    ag_send(A_ZF2, ZF)
    rs_wait(R_DB2, BB)
    dense_bwd(UP, xv.at[XB2], hv.at[HB2], zall.at[GB, me], total_of(BB), zall.at[ZB, me])
    ag_mid(A_ZF2, ZF)
    ag_send(A_G1, ZB)
    tables_wait(FW2)
    dispatch(A_ZF2, ZF, FW2, SF, False)
    experts_fwd(UP, SF, SF)
    w_first(LOW)
    ag_mid(A_G1, ZB)
    combine(R_F2, FB, FW2, SF, True)

    dispatch(A_G1, ZB, B1, RO, True)
    save_r1 = save(1, RO, r_o, 0)
    save_r1.start()
    load.wait()
    rs_mid(R_F2, FB)
    experts_bwd(LOW, SB, RO, SB)
    combine(R_DB1, BB, B1, SB, False, True)
    rs_mid(R_DB1, BB, True)
    rs_wait(R_F2, FB)
    block_out(FB, hv.at[HF], yv.at[LOW])
    send_y = rcopy(yv.at[LOW], y_o, o_s.at[LOW], o_r.at[LOW], stage_peer)
    send_y.start()
    save_r1.wait()

    def send_x(i, rows):
        return rcopy(yv.at[UP, rows], dx_o.at[rows], o_s.at[1 + i], o_r.at[1 + i], stage_peer)

    dense_bwd(LOW, xv.at[XB], hv.at[HB1], zall.at[ZB, me], total_of(BB), yv.at[UP], lambda k: rs_piece(R_DB1, BB, k), send_x)
    send_y.wait()
    for i in range(4):
        send_x(i, piece(i % 2, i // 2)).wait()


def weight_grads(z_ref, r_ref, dab_ref, mid_ref, y_ref, dx_ref, gg_ref, gu_ref, gd_ref, y_out, dx_out):
    y_out[0] = y_ref[...]
    dx_out[0] = dx_ref[...]
    for n in range(z_ref.shape[1]):
        dw = dot_tn(z_ref[0, n], dab_ref[0, n])
        gg_ref[0, 0, n] = dw[:, :F]
        gu_ref[0, 0, n] = dw[:, F:]
        gd_ref[0, 0, n] = dot_tn(mid_ref[0, n], r_ref[0, n])


def solution(mesh):
    def local_step(*args):
        arrays = [v[0] for v in args]
        route_fwd, gate_fwd, route_bwd, gate_bwd = arrays[8:]
        index = [v.transpose(0, 2, 1) for v in (route_bwd, route_fwd, gate_bwd, gate_fwd)]
        vmem, hbm = pl.BlockSpec(memory_space=pltpu.VMEM), pl.BlockSpec(memory_space=pl.ANY)
        dma = pltpu.SemaphoreType.DMA
        tok = jax.ShapeDtypeStruct((T, D), BF16)
        wide = jax.ShapeDtypeStruct((2, E, G * C, D), BF16)
        table = (4, G, 2, 16, 128)
        scratch = [(BF16, [(3, G, T, D), (3, E, G * C, D)]), (F32, [table, table]),
                   (BF16, [(2, D, FF), (2, FF, D), (3, T, D), (3, T, D), (2, T, D)]),
                   (F32, [(3, T, D), (2, 4, T, D), (2, 2, HALF, D), (2, 2, T, D)]),
                   (BF16, [(AHEAD + 1, Q, D, 2 * F), (AHEAD + 1, Q, F, D), (2, Q, G * C, D), (2, Q, G * C, F)])]
        gather, tables, sib, tree, last = (6, 10), (4, G), (5, 4), (5, 2, 2), (5, 2, 2, 2)
        sems = [gather, gather, tables, tables, sib, sib, tree, tree, last, last, (AHEAD + 1, 3), (2, 2), (5,), (5,), (5,)]
        outs = pl.pallas_call(
            kernel,
            out_shape=(tok, tok, wide, wide, wide, jax.ShapeDtypeStruct((2, E, G * C, F), BF16)),
            in_specs=[hbm] * 8 + [vmem] * 4,
            out_specs=(vmem, vmem, hbm, hbm, hbm, hbm),
            scratch_shapes=[pltpu.VMEM(shape, dtype) for dtype, shapes in scratch for shape in shapes] + [dma(shape) for shape in sems],
            compiler_params=pltpu.CompilerParams(collective_id=0, has_side_effects=True, vmem_limit_bytes=67043328),
        )(*arrays[:8], *index)
        y_next, dx_prev, z, r, dab, mid = outs
        q = 16
        rows = [pl.BlockSpec((1, q, G * C, w), lambda b, i: (b, i, 0, 0)) for w in (D, D, D, F)]
        up = jax.ShapeDtypeStruct((1, 2, E, D, F), F32)
        down = jax.ShapeDtypeStruct((1, 2, E, F, D), F32)
        up_spec = pl.BlockSpec((1, 1, q, D, F), lambda b, i: (0, b, i, 0, 0))
        down_spec = pl.BlockSpec((1, 1, q, F, D), lambda b, i: (0, b, i, 0, 0))
        tok_in = pl.BlockSpec((T, D), lambda b, i: (0, 0))
        tok_out = pl.BlockSpec((1, T, D), lambda b, i: (0, 0, 0))
        tok_full = jax.ShapeDtypeStruct((1, T, D), BF16)
        dgate, dup, ddown, y_next, dx_prev = pl.pallas_call(
            weight_grads,
            grid=(2, E // q),
            out_shape=(up, up, down, tok_full, tok_full),
            in_specs=rows + [tok_in] * 2,
            out_specs=(up_spec, up_spec, down_spec, tok_out, tok_out),
        )(z, r, dab, mid, y_next, dx_prev)
        return y_next, dx_prev, dgate, dup, ddown

    tok_spec = P('pp', 'ep', None)
    dense_spec = P('pp', None, None, None)
    exp_spec = P('pp', None, 'ep', None, None)
    route_spec = P('pp', None, 'ep', None)
    return jax.shard_map(local_step, mesh=mesh, in_specs=(tok_spec, tok_spec, tok_spec, dense_spec, dense_spec, exp_spec, exp_spec, exp_spec, route_spec, route_spec, route_spec, route_spec), out_specs=(tok_spec, tok_spec, exp_spec, exp_spec, exp_spec), check_vma=False)
```

```python
import jax
import jax.numpy as jnp
from jax import lax
from jax.experimental import pallas as pl
from jax.experimental.pallas import tpu as pltpu
from jax.sharding import PartitionSpec as P

MESH = pl.DeviceIdType.MESH
EPS = 1e-6
F32, BF16, I32 = jnp.float32, jnp.bfloat16, jnp.int32
T, D, FF, K = 768, 256, 1024, 8
G, E, C, F = 8, 48, 32, 128
S = E * C
NJ = S // 128
HALF = T // 2
PIECE = HALF // 2
ROWS = 256
B1, FW1, B2, FW2 = range(4)
SIB, XN, YN, DIAG = 1, 2, 4, 6
LOW, UP = 0, 1
BB, FB = 0, 1
Q, AHEAD = 8, 2
STEPS = E // Q


def dot(a, b):
    return jnp.dot(a, b, preferred_element_type=F32)


def dot_nt(a, b):
    return lax.dot_general(a, b, (((1,), (1,)), ((), ())), preferred_element_type=F32)


def dot_tn(a, b):
    return lax.dot_general(a, b, (((0,), (0,)), ((), ())), preferred_element_type=F32)


def rms_norm(v):
    return v * lax.rsqrt(jnp.mean(v * v, axis=-1, keepdims=True) + EPS)


def rms_back(v, g):
    inv = lax.rsqrt(jnp.mean(v * v, axis=-1, keepdims=True) + EPS)
    proj = jnp.mean(g * v, axis=-1, keepdims=True)
    return inv * g - v * (inv * inv * inv) * proj


def xor1(a, b):
    return a + b - 2 * a * b


def kernel(xf_h, xb_h, gin_h, win_h, wout_h, eg_h, eu_h, ed_h, rb_v, rf_v, gb_v, gf_v,
           y_o, dx_o, z_o, r_o, dab_o, mid_o,
           zall, slots, trow, tb, w1, w2, xv, hv, yv,
           part, sib_in, tree_in, fin_in, wgu, wd, dab_v, mid_v,
           ag_s, ag_r, tb_s, tb_r, sb_s, sb_r, tr_s, tr_r, fi_s, fi_r,
           w_sem, g_sem, l_sem, o_s, o_r):
    pp, me = lax.axis_index("pp"), lax.axis_index("ep")
    my_y, my_x, my_c = lax.div(me, 4), lax.rem(lax.div(me, 2), 2), lax.rem(me, 2)
    ZB, ZF, GB = range(3)
    SB, SF, RO = range(3)
    XB, XF, XB2 = range(3)
    HB1, HF, HB2 = range(3)

    def peer(r):
        if isinstance(r, int):
            ry, rx, rc = r // 4, r // 2 % 2, r % 2
        else:
            ry, rx, rc = lax.div(r, 4), lax.rem(lax.div(r, 2), 2), lax.rem(r, 2)
        return xor1(my_y, ry) * 4 + xor1(my_x, rx) * 2 + xor1(my_c, rc)

    def dev(r):
        return {"pp": pp, "ep": peer(r)}

    def rcopy(src, dst, s_sem, r_sem, to):
        return pltpu.make_async_remote_copy(src_ref=src, dst_ref=dst, send_sem=s_sem, recv_sem=r_sem, device_id=to, device_id_type=MESH)

    barrier = pltpu.get_barrier_semaphore()
    for r in range(1, G):
        pl.semaphore_signal(barrier, inc=1, device_id=dev(r), device_id_type=MESH)
    stage_peer = {"pp": 1 - pp, "ep": me}
    pl.semaphore_signal(barrier, inc=1, device_id=stage_peer, device_id_type=MESH)

    pairs = [(gin_h, zall.at[GB, me]), (xb_h, xv.at[XB]), (win_h, w1), (wout_h, w2), (xf_h, xv.at[XF])]
    local = [pltpu.make_async_copy(src, dst, l_sem.at[n]) for n, (src, dst) in enumerate(pairs)]
    for c in local:
        c.start()
    load_g, load_xb, load_w1, load_w2, load_xf = local

    def half(buf, r, h):
        return zall.at[buf, me if r is None else peer(r), pl.ds(h * HALF, HALF)]

    def ag_copy(i, n, ref, r):
        return rcopy(ref, ref, ag_s.at[i, n], ag_r.at[i, n], dev(r))

    X_LOW, X_UP, Y_LOW, Y_UP, OWN, D_LOW, D_UP, PASS = range(8)

    def ag_own(i, buf):
        low, up = half(buf, None, LOW), half(buf, None, UP)
        return [ag_copy(i, X_LOW, low, XN), ag_copy(i, Y_UP, up, YN), ag_copy(i, X_UP, up, XN), ag_copy(i, Y_LOW, low, YN),
                ag_copy(i, OWN, zall.at[buf, me], SIB)]

    def ag_pass(i, buf):
        return ag_copy(i, D_LOW, half(buf, XN, LOW), YN), ag_copy(i, D_UP, half(buf, YN, UP), XN)

    def ag_sib(i, buf, n):
        return ag_copy(i, PASS + n, zall.at[buf, peer((XN, YN, DIAG)[n])], SIB)

    def ag_send(i, buf, parts=slice(None)):
        for c in ag_own(i, buf)[parts]:
            c.start()

    def ag_mid(i, buf):
        first, second = ag_pass(i, buf)
        ag_copy(i, X_LOW, half(buf, XN, LOW), XN).wait_recv()
        first.start()
        ag_copy(i, Y_UP, half(buf, YN, UP), YN).wait_recv()
        second.start()

    def ag_step(i, buf, r):
        waits = [[(OWN, zall.at[buf, peer(SIB)]), (X_UP, half(buf, XN, UP))],
                 [(PASS, zall.at[buf, peer(XN + SIB)]), (Y_LOW, half(buf, YN, LOW))],
                 [(PASS + 1, zall.at[buf, peer(YN + SIB)]), (D_LOW, half(buf, DIAG, LOW)), (D_UP, half(buf, DIAG, UP))],
                 [(PASS + 2, zall.at[buf, peer(DIAG + SIB)])]]
        for n, group in enumerate(waits):
            @pl.when(r == 2 * n + 1)
            def _(n=n, group=group):
                for sem, ref in group:
                    ag_copy(i, sem, ref, SIB).wait_recv()
                if len(group) > 1:
                    ag_sib(i, buf, n).start()

    def ag_finish(i, buf):
        for c in ag_own(i, buf) + list(ag_pass(i, buf)):
            c.wait_send()
        for n in range(3):
            ag_sib(i, buf, n).wait_send()

    def dense_fwd(blk, x_ref, h_ref, z_ref):
        def body(i, _):
            rows = pl.ds(pl.multiple_of(i * ROWS, ROWS), ROWS)
            x = x_ref[rows, :].astype(F32)
            pre = dot(rms_norm(x).astype(BF16), w1[blk])
            h = (x + dot(jax.nn.silu(pre).astype(BF16), w2[blk])).astype(BF16)
            h_ref[rows, :] = h
            z_ref[rows, :] = rms_norm(h.astype(F32)).astype(BF16)
            return 0
        lax.fori_loop(0, T // ROWS, body, 0)

    def silu_grad(a):
        sig = jax.nn.sigmoid(a)
        return sig * (1.0 + a * (1.0 - sig))

    def dense_bwd(blk, x_ref, h_ref, g_ref, total, out_ref, before=None, after=None):
        def body(i, _):
            k, h = lax.div(i, 2), lax.rem(i, 2)
            if before is not None:
                @pl.when(h == 0)
                def _():
                    before(k)
            rows = piece(h, k)
            x = x_ref[rows, :].astype(F32)
            pre = dot(rms_norm(x).astype(BF16), w1[blk])
            dh = g_ref[rows, :].astype(F32) + rms_back(h_ref[rows, :].astype(F32), total(rows))
            dm = dot_nt(dh.astype(BF16), w2[blk])
            dp = (dm * silu_grad(pre)).astype(BF16)
            out_ref[rows, :] = (dh + rms_back(x, dot_nt(dp, w1[blk]))).astype(BF16)
            if after is not None:
                after(i, rows).start()
            return 0
        lax.fori_loop(0, 4, body, 0)

    def build_tables(ch, blk):
        rt = ch + 2 * blk
        route_ref, gate_ref = ((rb_v, gb_v), (rf_v, gf_v))[ch]

        def body(_, carry):
            acc_i = jnp.zeros((128, 128), F32)
            acc_g = jnp.zeros((128, 128), F32)
            for tc in range(T // 256):
                rows = route_ref[blk, :, tc * 256:(tc + 1) * 256]
                gates = gate_ref[blk, :, tc * 256:(tc + 1) * 256].astype(F32)
                cols, gcols = rows.T, gates.T
                quad = lax.shift_right_logical(rows, 7)
                place = quad + 4 * lax.shift_right_logical(quad * 43, 9)
                lane = lax.bitwise_and(cols, 127)
                tok = lax.broadcasted_iota(I32, (256, 128), 0) + (tc * 256 + 1)
                low = lax.bitwise_and(tok, 255)
                high = (tok - low).astype(F32)
                low = low.astype(F32)
                lanes = lax.broadcasted_iota(I32, (256, 128), 1)
                spots = lax.broadcasted_iota(I32, (128, 256), 0)
                for k in range(K):
                    a = jnp.where(spots == place[k:k + 1, :], 1.0, 0.0).astype(BF16)
                    hit = lanes == lane[:, k:k + 1]
                    b = jnp.concatenate([jnp.where(hit, low, 0.0), jnp.where(hit, high, 0.0)], axis=1).astype(BF16)
                    both = dot(a, b)
                    acc_i += both[:, :128] + both[:, 128:]
                    acc_g += dot(a, jnp.where(hit, gcols[:, k:k + 1], 0.0).astype(BF16))
            trow[rt, :, 0] = acc_i.reshape(G, 16, 128)
            trow[rt, :, 1] = acc_g.reshape(G, 16, 128)
            tb[rt, me] = trow[rt, me]
            return carry
        lax.fori_loop(0, 1, body, 0)

    def tables_send(rt):
        for r in range(1, G):
            rcopy(trow.at[rt, peer(r)], tb.at[rt, me], tb_s.at[rt, r], tb_r.at[rt, r], dev(r)).start()

    def tables_wait(rt):
        for r in range(1, G):
            rcopy(trow.at[rt, peer(r)], tb.at[rt, peer(r)], tb_s.at[rt, r], tb_r.at[rt, r], dev(r)).wait()

    def dispatch(ag, buf, rt, dst, gated):
        def body(r, _):
            if ag is not None:
                ag_step(ag, buf, r)
            src = peer(r)
            z = zall[buf, src]
            cols = tb[rt, src, 0].T
            gcols = tb[rt, src, 1].T if gated else None
            base = pl.multiple_of(src * C, C)
            want = lax.broadcasted_iota(I32, (128, T), 1).astype(F32) + 1.0
            for j in range(0, NJ, 4):
                parts = []
                for q in range(j, j + 4):
                    val = gcols[:, q:q + 1] if gated else 1.0
                    parts.append(jnp.where(want == cols[:, q:q + 1], val, 0.0).astype(BF16))
                got = dot(jnp.concatenate(parts, axis=0), z).astype(BF16)
                slots[dst, 4 * j:4 * j + 16, pl.ds(base, C), :] = got.reshape(16, C, D)
            return 0
        lax.fori_loop(0, G, body, 0)
        if ag is not None:
            ag_finish(ag, buf)

    def w_copies(blk, i):
        slot = i % (AHEAD + 1) if isinstance(i, int) else lax.rem(i, AHEAD + 1)
        es = pl.ds(i * Q, Q)
        return [pltpu.make_async_copy(eg_h.at[blk, es], wgu.at[slot, :, :, pl.ds(0, F)], w_sem.at[slot, 0]),
                pltpu.make_async_copy(eu_h.at[blk, es], wgu.at[slot, :, :, pl.ds(F, F)], w_sem.at[slot, 1]),
                pltpu.make_async_copy(ed_h.at[blk, es], wd.at[slot], w_sem.at[slot, 2])]

    def w_first(blk):
        for i in range(AHEAD):
            for c in w_copies(blk, i):
                c.start()

    def w_next(blk, i):
        @pl.when(i + AHEAD < STEPS)
        def _():
            for c in w_copies(blk, i + AHEAD):
                c.start()
        for c in w_copies(blk, i):
            c.wait()
        return lax.rem(i, AHEAD + 1)

    def experts_fwd(blk, src, dst):
        def body(i, _):
            slot = w_next(blk, i)
            es = [i * Q + n for n in range(Q)]
            gus = [dot(slots[src, e], wgu[slot, n]) for n, e in enumerate(es)]
            mids = [(jax.nn.silu(gu[:, :F]) * gu[:, F:]).astype(BF16) for gu in gus]
            outs = [dot(mid, wd[slot, n]).astype(BF16) for n, mid in enumerate(mids)]
            for e, out in zip(es, outs):
                slots[dst, e] = out
            return 0
        lax.fori_loop(0, STEPS, body, 0)

    def g_copies(blk, i, slot):
        es = pl.ds(i * Q, Q)
        return [pltpu.make_async_copy(dab_v.at[slot], dab_o.at[blk, es], g_sem.at[slot, 0]),
                pltpu.make_async_copy(mid_v.at[slot], mid_o.at[blk, es], g_sem.at[slot, 1])]

    def experts_bwd(blk, zsrc, rsrc, dst):
        def body(i, _):
            slot, spare = w_next(blk, i), lax.rem(i, 2)

            @pl.when(i >= 2)
            def _():
                for c in g_copies(blk, i - 2, spare):
                    c.wait()
            es = [i * Q + n for n in range(Q)]
            gus = [dot(slots[zsrc, e], wgu[slot, n]) for n, e in enumerate(es)]
            dms = [dot_nt(slots[rsrc, e], wd[slot, n]) for n, e in enumerate(es)]
            dabs = []
            for n in range(Q):
                a, b, dm = gus[n][:, :F], gus[n][:, F:], dms[n]
                sig = jax.nn.sigmoid(a)
                act = a * sig
                mid_v[spare, n] = (act * b).astype(BF16)
                da = (dm * b * (sig * (1.0 + a * (1.0 - sig)))).astype(BF16)
                dabs.append(jnp.concatenate([da, (dm * act).astype(BF16)], axis=1))
            outs = [dot_nt(dab, wgu[slot, n]).astype(BF16) for n, dab in enumerate(dabs)]
            for n, e in enumerate(es):
                dab_v[spare, n] = dabs[n]
                slots[dst, e] = outs[n]
            for c in g_copies(blk, i, spare):
                c.start()
            return 0
        lax.fori_loop(0, STEPS, body, 0)
        for i in (STEPS - 2, STEPS - 1):
            for c in g_copies(blk, i, i % 2):
                c.wait()

    def combine(rs, ch, rt, src, gated, tail=False):
        def rows_of(s):
            vals = slots[src, :, pl.ds(pl.multiple_of(s * C, C), C), :].reshape(S, D)
            want = lax.broadcasted_iota(I32, (T, 128), 0).astype(F32) + 1.0
            parts = []
            for j in range(NJ):
                val = tb[rt, s, 1, j:j + 1, :] if gated else 1.0
                parts.append(jnp.where(want == tb[rt, s, 0, j:j + 1, :], val, 0.0).astype(BF16))
            return dot(jnp.concatenate(parts, axis=1), vals)

        def sib_copy(q, n):
            return rcopy(part.at[n], sib_in.at[ch, q], sb_s.at[rs, q], sb_r.at[rs, q], dev(1))

        def body(m, _):
            first, last = 1 - lax.div(m + 6, 7), lax.div(m, 7)
            sib = lax.rem(m, 2) + first - last
            n = sib * lax.div(m + 1, 2) + (1 - sib) * (lax.div(m, 2) - 1 + last)
            q, spare = 3 - n, lax.rem(n, 2)

            @pl.when((sib == 1) & (n >= 2))
            def _():
                sib_copy(q + 2, spare).wait_send()
            part[sib * spare + (1 - sib) * 2] = rows_of(peer(2 * q + sib))

            @pl.when(sib == 1)
            def _():
                sib_copy(q, spare).start()

            @pl.when(sib == 0)
            def _():
                sib_copy(q, spare).wait_recv()
                sib_in[ch, q] += part[2]

            @pl.when(m == 2)
            def _():
                for k in range(2):
                    for c in tree(rs, ch, k):
                        c.start()

            if not tail:
                for step, axis, h in ((4, 1, UP), (6, 0, LOW)):
                    @pl.when(m == step)
                    def _(axis=axis, h=h):
                        for k in range(2):
                            fin(rs, ch, axis, h, k).start()
            return 0
        lax.fori_loop(0, 8, body, 0)
        for n in (2, 3):
            sib_copy(3 - n, n % 2).wait_send()

    def piece(h, k):
        return pl.ds(pl.multiple_of(h * HALF + k * PIECE, PIECE), PIECE)

    def rs_mid(rs, ch, tail=False):
        for k in range(2):
            for h, c in enumerate(tree(rs, ch, k)):
                c.wait()
                sib_in[ch, P_Y - h, piece(h, k)] += tree_in[ch, h, pl.ds(k * PIECE, PIECE)]
                fin(rs, ch, 1 - h, h, k).start()
            if tail:
                for h in range(2):
                    fin(rs, ch, h, h, k).start()

    P_OWN, P_X, P_Y, P_DIAG = range(4)

    def tree(rs, ch, k):
        return [rcopy(sib_in.at[ch, P_DIAG, piece(h, k)], tree_in.at[ch, h, pl.ds(k * PIECE, PIECE)],
                      tr_s.at[rs, h, k], tr_r.at[rs, h, k], dev(to)) for h, to in ((LOW, XN), (UP, YN))]

    def fin(rs, ch, axis, h, k):
        rows = piece(h, k)
        return rcopy(sib_in.at[ch, P_X + axis, rows], fin_in.at[ch, axis, rows], fi_s.at[rs, axis, h, k], fi_r.at[rs, axis, h, k], dev(2 + 2 * axis))

    def rs_piece(rs, ch, k):
        for axis in range(2):
            for h in range(2):
                fin(rs, ch, axis, h, k).wait()

    def rs_wait(rs, ch):
        for k in range(2):
            rs_piece(rs, ch, k)

    def total_of(ch):
        return lambda rows: sib_in[ch, P_OWN, rows, :] + fin_in[ch, 0, rows, :] + fin_in[ch, 1, rows, :]

    def block_out(ch, h_ref, out_ref):
        total = total_of(ch)

        def body(i, _):
            rows = pl.ds(pl.multiple_of(i * ROWS, ROWS), ROWS)
            out_ref[rows, :] = (h_ref[rows, :].astype(F32) + total(rows)).astype(BF16)
            return 0
        lax.fori_loop(0, T // ROWS, body, 0)

    def save(n, slot_array, out, blk):
        return pltpu.make_async_copy(slots.at[slot_array], out.at[blk], l_sem.at[n])

    A_ZB1, A_ZF1, A_G2, A_ZB2, A_ZF2, A_G1 = range(6)
    R_B1, R_F1, R_DB2, R_F2, R_DB1 = range(5)
    build_tables(BB, LOW)
    load_g.wait()
    pl.semaphore_wait(barrier, G)
    tables_send(B1)
    ag_send(A_G2, GB, slice(2))
    w_first(LOW)
    for c in (load_xb, load_w1, load_w2):
        c.wait()
    dense_fwd(LOW, xv.at[XB], hv.at[HB1], zall.at[ZB, me])
    ag_send(A_ZB1, ZB)
    build_tables(FB, LOW)
    tables_send(FW1)
    load_xf.wait()
    dense_fwd(LOW, xv.at[XF], hv.at[HF], zall.at[ZF, me])
    ag_mid(A_ZB1, ZB)
    ag_send(A_ZF1, ZF)
    build_tables(BB, UP)
    build_tables(FB, UP)
    tables_send(B2)
    tables_send(FW2)

    tables_wait(B1)
    dispatch(A_ZB1, ZB, B1, SB, False)
    save_z1 = save(0, SB, z_o, 0)
    save_z1.start()
    ag_mid(A_ZF1, ZF)
    ag_send(A_G2, GB, slice(2, None))
    experts_fwd(LOW, SB, RO)
    w_first(LOW)
    combine(R_B1, BB, B1, RO, True)

    tables_wait(FW1)
    dispatch(A_ZF1, ZF, FW1, SF, False)
    rs_mid(R_B1, BB)
    ag_mid(A_G2, GB)
    experts_fwd(LOW, SF, SF)
    w_first(UP)
    rs_wait(R_B1, BB)
    block_out(BB, hv.at[HB1], xv.at[XB2])
    dense_fwd(UP, xv.at[XB2], hv.at[HB2], zall.at[ZB, me])
    ag_send(A_ZB2, ZB)
    tables_wait(B2)
    dispatch(A_G2, GB, B2, RO, True)
    save_r2 = save(1, RO, r_o, 1)
    save_r2.start()
    ag_mid(A_ZB2, ZB)
    combine(R_F1, FB, FW1, SF, True)
    save_z1.wait()
    dispatch(A_ZB2, ZB, B2, SB, False)
    rs_mid(R_F1, FB)
    save_z2 = save(2, SB, z_o, 1)
    save_z2.start()
    save_r2.wait()
    experts_bwd(UP, SB, RO, RO)
    w_first(UP)
    save_z2.wait()
    load = pltpu.make_async_copy(z_o.at[LOW], slots.at[SB], l_sem.at[3])
    load.start()
    combine(R_DB2, BB, B2, RO, False)

    rs_wait(R_F1, FB)
    block_out(FB, hv.at[HF], xv.at[XF])
    dense_fwd(UP, xv.at[XF], hv.at[HF], zall.at[ZF, me])
    rs_mid(R_DB2, BB)
    ag_send(A_ZF2, ZF)
    rs_wait(R_DB2, BB)
    dense_bwd(UP, xv.at[XB2], hv.at[HB2], zall.at[GB, me], total_of(BB), zall.at[ZB, me])
    ag_mid(A_ZF2, ZF)
    ag_send(A_G1, ZB)
    tables_wait(FW2)
    dispatch(A_ZF2, ZF, FW2, SF, False)
    experts_fwd(UP, SF, SF)
    w_first(LOW)
    ag_mid(A_G1, ZB)
    combine(R_F2, FB, FW2, SF, True)

    dispatch(A_G1, ZB, B1, RO, True)
    save_r1 = save(1, RO, r_o, 0)
    save_r1.start()
    load.wait()
    rs_mid(R_F2, FB)
    experts_bwd(LOW, SB, RO, SB)
    combine(R_DB1, BB, B1, SB, False, True)
    rs_mid(R_DB1, BB, True)
    rs_wait(R_F2, FB)
    block_out(FB, hv.at[HF], yv.at[LOW])
    send_y = rcopy(yv.at[LOW], y_o, o_s.at[LOW], o_r.at[LOW], stage_peer)
    send_y.start()
    save_r1.wait()

    def send_x(i, rows):
        return rcopy(yv.at[UP, rows], dx_o.at[rows], o_s.at[1 + i], o_r.at[1 + i], stage_peer)

    dense_bwd(LOW, xv.at[XB], hv.at[HB1], zall.at[ZB, me], total_of(BB), yv.at[UP], lambda k: rs_piece(R_DB1, BB, k), send_x)
    send_y.wait()
    for i in range(4):
        send_x(i, piece(i % 2, i // 2)).wait()


def weight_grads(z_ref, r_ref, dab_ref, mid_ref, y_ref, dx_ref, gg_ref, gu_ref, gd_ref, y_out, dx_out):
    y_out[0] = y_ref[...]
    dx_out[0] = dx_ref[...]
    for n in range(z_ref.shape[1]):
        dw = dot_tn(z_ref[0, n], dab_ref[0, n])
        gg_ref[0, 0, n] = dw[:, :F]
        gu_ref[0, 0, n] = dw[:, F:]
        gd_ref[0, 0, n] = dot_tn(mid_ref[0, n], r_ref[0, n])


def solution(mesh):
    def local_step(*args):
        arrays = [v[0] for v in args]
        route_fwd, gate_fwd, route_bwd, gate_bwd = arrays[8:]
        index = [v.transpose(0, 2, 1) for v in (route_bwd, route_fwd, gate_bwd, gate_fwd)]
        vmem, hbm = pl.BlockSpec(memory_space=pltpu.VMEM), pl.BlockSpec(memory_space=pl.ANY)
        dma = pltpu.SemaphoreType.DMA
        tok = jax.ShapeDtypeStruct((T, D), BF16)
        wide = jax.ShapeDtypeStruct((2, E, G * C, D), BF16)
        table = (4, G, 2, 16, 128)
        scratch = [(BF16, [(3, G, T, D), (3, E, G * C, D)]), (F32, [table, table]),
                   (BF16, [(2, D, FF), (2, FF, D), (3, T, D), (3, T, D), (2, T, D)]),
                   (F32, [(3, T, D), (2, 4, T, D), (2, 2, HALF, D), (2, 2, T, D)]),
                   (BF16, [(AHEAD + 1, Q, D, 2 * F), (AHEAD + 1, Q, F, D), (2, Q, G * C, D), (2, Q, G * C, F)])]
        gather, tables, sib, tree, last = (6, 10), (4, G), (5, 4), (5, 2, 2), (5, 2, 2, 2)
        sems = [gather, gather, tables, tables, sib, sib, tree, tree, last, last, (AHEAD + 1, 3), (2, 2), (5,), (5,), (5,)]
        outs = pl.pallas_call(
            kernel,
            out_shape=(tok, tok, wide, wide, wide, jax.ShapeDtypeStruct((2, E, G * C, F), BF16)),
            in_specs=[hbm] * 8 + [vmem] * 4,
            out_specs=(vmem, vmem, hbm, hbm, hbm, hbm),
            scratch_shapes=[pltpu.VMEM(shape, dtype) for dtype, shapes in scratch for shape in shapes] + [dma(shape) for shape in sems],
            compiler_params=pltpu.CompilerParams(collective_id=0, has_side_effects=True, vmem_limit_bytes=67043328),
        )(*arrays[:8], *index)
        y_next, dx_prev, z, r, dab, mid = outs
        q = 16
        rows = [pl.BlockSpec((1, q, G * C, w), lambda b, i: (b, i, 0, 0)) for w in (D, D, D, F)]
        up = jax.ShapeDtypeStruct((1, 2, E, D, F), F32)
        down = jax.ShapeDtypeStruct((1, 2, E, F, D), F32)
        up_spec = pl.BlockSpec((1, 1, q, D, F), lambda b, i: (0, b, i, 0, 0))
        down_spec = pl.BlockSpec((1, 1, q, F, D), lambda b, i: (0, b, i, 0, 0))
        tok_in = pl.BlockSpec((T, D), lambda b, i: (0, 0))
        tok_out = pl.BlockSpec((1, T, D), lambda b, i: (0, 0, 0))
        tok_full = jax.ShapeDtypeStruct((1, T, D), BF16)
        dgate, dup, ddown, y_next, dx_prev = pl.pallas_call(
            weight_grads,
            grid=(2, E // q),
            out_shape=(up, up, down, tok_full, tok_full),
            in_specs=rows + [tok_in] * 2,
            out_specs=(up_spec, up_spec, down_spec, tok_out, tok_out),
        )(z, r, dab, mid, y_next, dx_prev)
        return y_next, dx_prev, dgate, dup, ddown

    tok_spec = P('pp', 'ep', None)
    dense_spec = P('pp', None, None, None)
    exp_spec = P('pp', None, 'ep', None, None)
    route_spec = P('pp', None, 'ep', None)
    return jax.shard_map(local_step, mesh=mesh, in_specs=(tok_spec, tok_spec, tok_spec, dense_spec, dense_spec, exp_spec, exp_spec, exp_spec, route_spec, route_spec, route_spec, route_spec), out_specs=(tok_spec, tok_spec, exp_spec, exp_spec, exp_spec), check_vma=False)
```
